256 devices in a mesh: tile: 64 (over y, z, core), row: 4 (over x).
Axes of the slice: x: 4, y: 4, z: 8, core: 2. Of those that a mesh axis runs over, the one named last changes fastest.
Arguments:
- intensity: bfloat16 [64, 128, 11264], P('tile', 'row'), may hold values from 0.099609375 to 1
- volume: float32 [512, 128, 256], P('tile', 'row'), may hold values from 0 to 1
- footprint: bfloat16 [64, 256, 256], P('tile'), may hold values from 0.0001335144 to 0.0026855469
- foot_offset: int32 [512, 64], replicated, may hold values from 2 to 84, as said below
- tile_count: int32 [64], replicated, may hold values from 1 to 8, as said below
Outputs:
- residual: float32 [64, 128, 11264], P('tile', 'row')
- correction: float32 [512, 128, 256], P('tile', 'row')
The draws below stay inside these ranges and needn't reach their ends.
Inputs may be any that keep to these rules, and one draw needn't show every extreme that they name: `foot_offset`: slot j belongs to group j // 8. At every angle the offsets of one group's slots differ by at most 3; wherever a group has two or more slots, by exactly 3. `tile_count`: some group has all its slots live.
All inputs are finite; a program needn't handle non-finite values.
Results may differ from the reference program's by a relative error of at most 0.00065.
Values may be sent and summed in bfloat16 or wider, within the bound.
A program may use at most 128 MiB of HBM per device.

```python
import math
import jax
import jax.numpy as jnp
import numpy as np
from jax import lax

NCB = 88
CB = 128
TV = 256
SPREAD = 4
RIM = 3
SLOTS_DEV = 8
ANGLES = 64
ROWS = 128
TILE_SLOTS = 512
GROUPS = 64


def draw_foot_offset(key, part):
    base_key = jax.random.fold_in(key, 11)
    first_key, second_key, third_key = jax.random.split(base_key, 3)
    starts = jax.random.randint(first_key, (GROUPS, 1, ANGLES), 2, NCB - SPREAD - 2, dtype=jnp.int32)
    deltas = jax.random.randint(second_key, (GROUPS, SLOTS_DEV, ANGLES), 0, SPREAD, dtype=jnp.int32)
    slot_ids = jnp.arange(SLOTS_DEV, dtype=jnp.int32)[None, :, None]
    scores = jax.random.randint(third_key, (GROUPS, SLOTS_DEV, ANGLES), 0, 1 << 20, dtype=jnp.int32) * SLOTS_DEV + slot_ids
    ranked = jnp.argsort(scores, axis=1, stable=True).astype(jnp.int32)
    lowest = ranked[:, 0:1, :]
    highest = ranked[:, min(1, SLOTS_DEV - 1):min(2, SLOTS_DEV), :]
    deltas = jnp.where(slot_ids == highest, SPREAD - 1, deltas)
    deltas = jnp.where(slot_ids == lowest, 0, deltas)
    return (starts + deltas).reshape(TILE_SLOTS, ANGLES)


def draw_tile_count(key, part):
    base_key = jax.random.fold_in(key, 23)
    first_key, second_key = jax.random.split(base_key)
    counts = jax.random.randint(first_key, (GROUPS,), 1, SLOTS_DEV + 1, dtype=jnp.int32)
    fullest = jax.random.randint(second_key, (), 0, GROUPS, dtype=jnp.int32)
    return jnp.where(jnp.arange(GROUPS, dtype=jnp.int32) == fullest, SLOTS_DEV, counts)


def shard_levels(own_key, extent, shards, least, largest):
    factor_of = 1.0
    for dim, parts in shards:
        steps = jax.random.uniform(jax.random.fold_in(jax.random.fold_in(own_key, 6), dim), (parts,), jnp.float32, least / len(shards), largest / len(shards))
        factor_of = factor_of * jnp.repeat(jnp.exp(steps), extent[dim] // parts).reshape((-1,) + (1,) * (len(extent) - 1 - dim))
    return factor_of


def setup_inputs(seed: int = 0) -> dict:
    keys = jax.random.split(jax.random.key(seed), 6)
    return {
        "intensity": jnp.clip(jnp.exp(math.log(1.0) - 2.306499 * jax.random.uniform(keys[0], (ANGLES, ROWS, NCB * CB), jnp.float32) ** shard_levels(keys[0], (ANGLES, ROWS, NCB * CB), ((0, 64), (1, 4)), -0.2, 0.2)), 0.099609375, 1.0).astype(jnp.bfloat16),
        "volume": jnp.clip(1.0 * jax.random.uniform(keys[1], (TILE_SLOTS, ROWS, TV), jnp.float32) ** shard_levels(keys[1], (TILE_SLOTS, ROWS, TV), ((0, 64), (1, 4)), -0.2, 0.2), 0.0, 1.0),
        "footprint": jnp.clip(jnp.exp(math.log(0.0026855469) - 3.0014303 * jax.random.uniform(keys[2], (ANGLES, TV, 2 * CB), jnp.float32) ** shard_levels(keys[2], (ANGLES, TV, 2 * CB), ((0, 64),), -0.2, 0.2)), 0.0001335144, 0.0026855469).astype(jnp.bfloat16),
        "foot_offset": draw_foot_offset(jax.random.fold_in(keys[5], 71), 0),
        "tile_count": draw_tile_count(jax.random.fold_in(keys[5], 71), 0),
    }


decay_length = 2.0
row_floor = 0.5


def smoothing_taps():
    spread_taps = np.exp(-np.abs(np.arange(-RIM, RIM + 1)) / decay_length)
    return spread_taps / spread_taps.sum()


def retrieve_phase(intensity):
    tap_weights = smoothing_taps()
    height_rows = intensity.shape[1]
    column_count = intensity.shape[2]
    padded = jnp.pad(intensity.astype(jnp.float32), ((0, 0), (RIM, RIM), (0, 0)))
    across = float(tap_weights[0]) * padded[:, 0:height_rows, :]
    for tap_index in range(1, 2 * RIM + 1):
        across = across + float(tap_weights[tap_index]) * padded[:, tap_index:tap_index + height_rows, :]
    widened = jnp.pad(across, ((0, 0), (0, 0), (RIM, RIM)))
    smoothed = float(tap_weights[0]) * widened[:, :, 0:column_count]
    for tap_index in range(1, 2 * RIM + 1):
        smoothed = smoothed + float(tap_weights[tap_index]) * widened[:, :, tap_index:tap_index + column_count]
    return -jnp.log(smoothed)


def reference(intensity, volume, footprint, foot_offset, tile_count):
    phase_map = retrieve_phase(intensity)
    slot_ids = jnp.arange(TILE_SLOTS, dtype=jnp.int32)
    repeated = jnp.broadcast_to(tile_count[:, None], (GROUPS, SLOTS_DEV)).reshape(TILE_SLOTS)
    live = (slot_ids % SLOTS_DEV < repeated).astype(jnp.float32)
    masked = volume * live[:, None, None]
    table_all = footprint.astype(jnp.float32)
    column_sums = jnp.sum(table_all, axis=(0, 2))
    block_ids = jnp.arange(NCB, dtype=jnp.int32)

    def one_angle(running, inputs):
        table_one, offsets, phase_one = inputs
        load_blocks = jax.ops.segment_sum(masked, offsets, num_segments=NCB)
        load_half = lax.optimization_barrier(load_blocks.astype(jnp.bfloat16)).astype(jnp.float32)
        images = jnp.einsum('brv,vc->rbc', load_half, table_one)
        leading = images[:, :, :CB]
        trailing = jnp.concatenate([jnp.zeros_like(images[:, :1, CB:]), images[:, :-1, CB:]], axis=1)
        projection = (leading + trailing).reshape(ROWS, NCB * CB)
        voxel_sums = jnp.sum(table_one, axis=0)
        counts = jnp.sum((offsets[:, None] == block_ids[None, :]).astype(jnp.float32) * live[:, None], axis=0)
        row_first = counts[:, None] * voxel_sums[None, :CB]
        row_second = counts[:, None] * voxel_sums[None, CB:]
        row_second = jnp.concatenate([jnp.zeros_like(row_second[:1]), row_second[:-1]], axis=0)
        row_sums = (row_first + row_second).reshape(NCB * CB)
        residual = phase_one - projection
        weighted = lax.optimization_barrier((residual / jnp.maximum(row_sums, row_floor)).astype(jnp.bfloat16)).astype(jnp.float32)
        halves = weighted.reshape(ROWS, NCB, CB)
        nearer = jnp.einsum('rbc,vc->brv', halves, table_one[:, :CB])
        farther = jnp.einsum('rbc,vc->brv', halves, table_one[:, CB:])
        farther = jnp.concatenate([farther[1:], jnp.zeros_like(farther[:1])], axis=0)
        back_blocks = nearer + farther
        running = running + jnp.take(back_blocks, offsets, axis=0)
        return running, residual

    start_sum = jnp.zeros((TILE_SLOTS, ROWS, TV), jnp.float32)
    summed, residual = lax.scan(one_angle, start_sum, (table_all, jnp.transpose(foot_offset), phase_map))
    correction = summed * live[:, None, None] / column_sums[None, None, :]
    return residual, correction
```

```python
import functools

import jax
import jax.numpy as jnp
import numpy as np
from jax import lax
from jax.experimental import pallas as pl
from jax.experimental.pallas import tpu as pltpu
from jax.sharding import PartitionSpec as P

RIM = 3
NCB = 88
CB = 128
TV = 256
YS, ZS, CS, XS = 4, 8, 2, 4
SLOTS = 8
RB = 8
SUB = RB * TV
TOTAL = YS * ZS * CS * SLOTS
BP = 96
ROWS_HERE = YS * RB

decay_length = 2.0
row_floor = 0.5

F32 = jnp.float32
BF16 = jnp.bfloat16
MESH = pl.DeviceIdType.MESH


def smoothing_taps():
    spread_taps = np.exp(-np.abs(np.arange(-RIM, RIM + 1)) / decay_length)
    return [float(t) for t in (spread_taps / spread_taps.sum()).astype(np.float32)]


def dot(a, b, dims=((1,), (0,))):
    return lax.dot_general(a, b, (dims, ((), ())), preferred_element_type=F32)


def kernel(
    inten, vol, foot, offm, offmt,
    res_out, cor_out, col_out,
    vol_s, vol_g, foot_g, cs_y, cs_g,
    halo_lo, halo_hi, rows_p, rows_a, ph_s, ph,
    hot, hot_t, loads, weigh, res_w, back, terms, pair_r, ring_r,
    y_send, y_recv, h_send, h_recv, g_send, g_recv, q_send, q_recv,
    p_send, p_recv, r_send, r_recv, l_sem,
):
    taps = smoothing_taps()
    t = lax.axis_index("tile")
    x = lax.axis_index("row")
    y = t // (ZS * CS)
    zc = t % (ZS * CS)
    z = zc // CS
    c = zc % CS

    def tile_of(yy, zz, cc):
        return (yy * ZS + zz) * CS + cc

    def device(yy, zz, cc):
        return (tile_of(yy, zz, cc), x)

    partner = device(y, z, 1 - c)
    right = device(y, (z + 1) % ZS, c)
    left = device(y, (z + ZS - 1) % ZS, c)
    toward = (right, left)
    y_peer = [(y + d) % YS for d in range(1, YS)]
    y_from = [(y + YS - d) % YS for d in range(1, YS)]
    x_up = (t, (x + 1) % XS)
    x_down = (t, (x + XS - 1) % XS)

    barrier = pltpu.get_barrier_semaphore()
    peers = [device(yy, z, c) for yy in y_peer] + [partner, right, left, x_up, x_down]
    for peer in peers:
        pl.semaphore_signal(barrier, inc=1, device_id=peer, device_id_type=MESH)
    pl.semaphore_wait(barrier, len(peers))

    started = []

    def send(src, dst, ssem, rsem, dev):
        copy = pltpu.make_async_remote_copy(
            src_ref=src, dst_ref=dst, send_sem=ssem, recv_sem=rsem,
            device_id=dev, device_id_type=MESH,
        )
        copy.start()
        started.append(copy)

    def arrive(dst, ssem, rsem, dev):
        pltpu.make_async_remote_copy(
            src_ref=dst, dst_ref=dst, send_sem=ssem, recv_sem=rsem,
            device_id=dev, device_id_type=MESH,
        ).wait_recv()

    def y_copy(kind, d, src, dst):
        send(src, dst, y_send.at[kind, d], y_recv.at[kind, d], device(y_peer[d], z, c))

    def y_wait(kind, d, dst):
        arrive(dst, y_send.at[kind, d], y_recv.at[kind, d], device(y_from[d], z, c))

    send(inten.at[0, pl.ds(ROWS_HERE - 8, 8), :], halo_lo, h_send.at[0], h_recv.at[0], x_up)
    send(inten.at[0, pl.ds(0, 8), :], halo_hi, h_send.at[1], h_recv.at[1], x_down)

    for q in range(YS):
        for r in range(RB):
            vol_s[q, :, r * TV : (r + 1) * TV] = vol[:, q * RB + r, :].astype(BF16)
    for d in range(3):
        y_copy(0, d, vol_s.at[y_peer[d]], vol_g.at[y, zc])
    ones = jnp.ones((8, TV), BF16)
    cs_y[y] = dot(ones, foot[0], ((1,), (1,)))
    for d in range(3):
        y_copy(1, d, cs_y.at[y], cs_y.at[y])
    for d in range(3):
        y_copy(2, d, foot.at[0], foot_g.at[y])
    vol_g[y, zc] = vol_s[y]
    foot_g[y] = foot[0]

    def chunk_of(zz, cc, p):
        return vol_g.at[pl.ds(2 * p, 2), zz * CS + cc]

    def give_partner(index, zz, p):
        src = chunk_of(zz, c, p)
        send(src, src, q_send.at[index, p], q_recv.at[index, p], partner)

    def give_partner_sums(index, zz):
        src = cs_g.at[zz * CS + c]
        send(src, src, q_send.at[index, 2], q_recv.at[index, 2], partner)

    def ring_send(way, step, p, zz):
        src = chunk_of(zz, c, p)
        send(src, src, g_send.at[way, step, p], g_recv.at[way, step, p], toward[way])

    def ring_wait(way, step, p, zz):
        arrive(chunk_of(zz, c, p), g_send.at[way, step, p], g_recv.at[way, step, p], toward[1 - way])

    def sums_send(way, step, zz):
        src = cs_g.at[zz * CS + c]
        send(src, src, g_send.at[way, step, 2], g_recv.at[way, step, 2], toward[way])

    def sums_wait(way, step, zz):
        arrive(cs_g.at[zz * CS + c], g_send.at[way, step, 2], g_recv.at[way, step, 2], toward[1 - way])

    for d in range(3):
        y_wait(0, d, vol_g.at[y_from[d], zc])
    for p in range(2):
        for way in range(2):
            ring_send(way, 0, p, z)
    for d in range(3):
        y_wait(1, d, cs_y.at[y_from[d]])
    cs_g[zc] = cs_y[0] + cs_y[1] + cs_y[2] + cs_y[3]
    for way in range(2):
        sums_send(way, 0, z)
    for p in range(2):
        give_partner(0, z, p)
    give_partner_sums(0, z)

    arrive(halo_lo, h_send.at[0], h_recv.at[0], x_down)
    arrive(halo_hi, h_send.at[1], h_recv.at[1], x_up)
    rows_a[0] = jnp.zeros((ROWS_HERE, CB), F32)
    rows_a[NCB + 1] = jnp.zeros((ROWS_HERE, CB), F32)
    has_lo = (x > 0).astype(F32)
    has_hi = (x < XS - 1).astype(F32)

    def vertical(b, _):
        cols = pl.ds(pl.multiple_of(b * CB, CB), CB)
        rows_p[b, 0:8, :] = halo_lo[:, cols].astype(F32) * has_lo
        rows_p[b, 8 : 8 + ROWS_HERE, :] = inten[0, :, cols].astype(F32)
        rows_p[b, 8 + ROWS_HERE : 16 + ROWS_HERE, :] = halo_hi[:, cols].astype(F32) * has_hi
        across = taps[RIM] * rows_p[b, 8 : 8 + ROWS_HERE, :]
        for k in range(1, RIM + 1):
            across = across + taps[RIM + k] * (
                rows_p[b, 8 - k : 8 - k + ROWS_HERE, :] + rows_p[b, 8 + k : 8 + k + ROWS_HERE, :]
            )
        rows_a[b + 1] = across
        return 0

    lax.fori_loop(0, NCB, vertical, 0)
    lane = lax.broadcasted_iota(jnp.int32, (ROWS_HERE, CB), 1)

    def horizontal(b, _):
        before, here, after = rows_a[b], rows_a[b + 1], rows_a[b + 2]
        smooth = taps[RIM] * here
        for k in range(1, RIM + 1):
            ahead = pltpu.roll(jnp.where(lane < k, after, here), CB - k, 1)
            behind = pltpu.roll(jnp.where(lane >= CB - k, before, here), k, 1)
            smooth = smooth + taps[RIM + k] * (ahead + behind)
        phase = -jnp.log(smooth)
        for q in range(YS):
            ph_s[q, pl.ds(pl.multiple_of(b * RB, RB), RB), :] = phase[q * RB : (q + 1) * RB]
        return 0

    lax.fori_loop(0, NCB, horizontal, 0)
    for d in range(3):
        y_copy(3, d, ph_s.at[y_peer[d]], ph.at[y])
    ph[y] = ph_s[y]

    for step in range(1, 5):
        for p in range(2):
            for way in range(2):
                if step == 4 and p != way:
                    continue
                zz = (z + ZS - step) % ZS if way == 0 else (z + step) % ZS
                ring_wait(way, step - 1, p, zz)
                if step < 3 or (step == 3 and p == way):
                    ring_send(way, step, p, zz)
                index = step if way == 0 or step == 4 else 4 + step
                give_partner(index, zz, p)
        for way in range(2):
            if step == 4 and way == 1:
                continue
            zz = (z + ZS - step) % ZS if way == 0 else (z + step) % ZS
            sums_wait(way, step - 1, zz)
            if step < 3 or (step == 3 and way == 0):
                sums_send(way, step, zz)
            give_partner_sums(step if way == 0 else 4 + step, zz)

    block = lax.broadcasted_iota(jnp.int32, (BP, TOTAL), 0)
    for i in range(YS):
        row = offmt[pl.ds(tile_of(i, z, c), 1), :]
        hot[i * BP : (i + 1) * BP, :] = (row == block).astype(F32).astype(BF16)
    angle = lax.broadcasted_iota(jnp.int32, (TOTAL, YS * ZS * CS), 1)
    block_t = lax.broadcasted_iota(jnp.int32, (TOTAL, CB), 1)
    for i in range(YS):
        col = jnp.sum(jnp.where(angle == tile_of(i, z, c), offm[...], 0), axis=1, keepdims=True)
        hot_t[:, i * CB : (i + 1) * CB] = (col == block_t).astype(F32).astype(BF16)
    for h in range(2):
        for i in range(YS):
            back[h, i * CB + BP : (i + 1) * CB, :] = jnp.zeros((CB - BP, SUB), BF16)

    for d in range(3):
        y_wait(2, d, foot_g.at[y_from[d]])
    for index in range(8):
        zz = (z + ZS - index) % ZS if index < 5 else (z + index - 4) % ZS
        for p in range(2):
            arrive(chunk_of(zz, 1 - c, p), q_send.at[index, p], q_recv.at[index, p], partner)
        arrive(cs_g.at[zz * CS + 1 - c], q_send.at[index, 2], q_recv.at[index, 2], partner)

    def load_row(r, _):
        cols = pl.ds(pl.multiple_of(r * TV, TV), TV)
        got = dot(hot[...], vol_g[:, :, :, cols].reshape(TOTAL, TV)).astype(BF16)
        for i in range(YS):
            loads[i, pl.ds(pl.multiple_of(r * BP, BP), BP), :] = got[i * BP : (i + 1) * BP]
        return 0

    lax.fori_loop(0, RB, load_row, 0)
    for d in range(3):
        y_wait(3, d, ph.at[y_from[d]])

    def one_angle(i, _):
        table = foot_g[i]
        counts = jnp.sum(hot[pl.ds(pl.multiple_of(i * BP, BP), BP), :].astype(F32), axis=1, keepdims=True)
        sums = dot(ones, table)[0:1]
        totals = counts * sums[:, :CB] + pltpu.roll(counts * sums[:, CB:], 1, 0)
        scale = (1.0 / jnp.maximum(totals, row_floor))[:NCB]
        images = dot(loads[i], table)
        for r in range(RB):
            image = images[r * BP : (r + 1) * BP]
            shadow = image[:, :CB] + pltpu.roll(image[:, CB:], 1, 0)
            left_over = ph[i, pl.ds(r, NCB, stride=RB), :] - shadow[:NCB]
            res_w[i, pl.ds(r, NCB, stride=RB), :] = left_over
            near = jnp.concatenate([left_over * scale, jnp.zeros((BP - NCB, CB), F32)], axis=0)
            far = pltpu.roll(near, BP - 1, 0)
            weigh[r * BP : (r + 1) * BP, :] = jnp.concatenate([near, far], axis=1).astype(BF16)
        spread = dot(weigh[...], table, ((1,), (1,)))
        rows = pl.ds(pl.multiple_of(i * CB, CB), BP)
        for r in range(RB):
            part = spread[r * BP : (r + 1) * BP]
            high = part.astype(BF16)
            back[0, rows, r * TV : (r + 1) * TV] = high
            back[1, rows, r * TV : (r + 1) * TV] = (part - high.astype(F32)).astype(BF16)
        return 0

    lax.fori_loop(0, YS, one_angle, 0)
    for d in range(3):
        y_copy(4, d, res_w.at[y_peer[d]], res_out.at[y])
    own_res = pltpu.make_async_copy(res_w.at[y], res_out.at[y], l_sem.at[0])
    own_res.start()

    def term_row(r, _):
        cols = pl.ds(pl.multiple_of(r * TV, TV), TV)
        got = dot(hot_t[...], back[0, :, cols]) + dot(hot_t[...], back[1, :, cols])
        terms[:, :, :, :, cols] = got.reshape(YS, ZS, CS, SLOTS, TV)
        return 0

    lax.fori_loop(0, RB, term_row, 0)

    order = (4, 3, 5, 2, 6, 1, 7, 0)
    for off in order:
        zz = (z + off) % ZS
        send(terms.at[:, zz, 1 - c], pair_r.at[zz], p_send.at[off], p_recv.at[off], partner)

    def add_pair(off):
        zz = (z + off) % ZS
        arrive(pair_r.at[zz], p_send.at[off], p_recv.at[off], partner)
        terms[:, zz, c] = terms[:, zz, c] + pair_r[zz]

    def sum_send(way, step, p, zz):
        send(
            terms.at[pl.ds(2 * p, 2), zz, c], ring_r.at[way, step, p],
            r_send.at[way, step, p], r_recv.at[way, step, p], toward[way],
        )

    def sum_wait(way, step, p):
        arrive(ring_r.at[way, step, p], r_send.at[way, step, p], r_recv.at[way, step, p], toward[1 - way])

    for step in range(4):
        for way in range(2):
            if step > 0 or way == 0:
                add_pair(4 - step if way == 0 else 4 + step)
        for p in range(2):
            for way in range(2):
                if step == 0 and p != way:
                    continue
                zz = (z + 4 - step) % ZS if way == 0 else (z + 4 + step) % ZS
                if step > 1 or (step == 1 and p == way):
                    sum_wait(way, step - 1, p)
                    half = pl.ds(2 * p, 2)
                    terms[half, zz, c] = terms[half, zz, c] + ring_r[way, step - 1, p]
                sum_send(way, step, p, zz)
    add_pair(0)
    for p in range(2):
        half = pl.ds(2 * p, 2)
        for way in range(2):
            sum_wait(way, 3, p)
            terms[half, z, c] = terms[half, z, c] + ring_r[way, 3, p]
    for d in range(3):
        y_copy(5, d, terms.at[y_peer[d], z, c], cor_out.at[y])
    own_cor = pltpu.make_async_copy(terms.at[y, z, c], cor_out.at[y], l_sem.at[1])
    own_cor.start()
    total = cs_g[0]
    for k in range(1, ZS * CS):
        total = total + cs_g[k]
    col_out[...] = total

    for d in range(3):
        y_wait(4, d, res_out.at[y_from[d]])
    for d in range(3):
        y_wait(5, d, cor_out.at[y_from[d]])
    own_res.wait()
    own_cor.wait()
    for copy in started:
        copy.wait_send()


def local(intensity, volume, footprint, foot_offset, tile_count):
    live = (jnp.arange(SLOTS, dtype=jnp.int32)[None, :] < tile_count[:, None]).reshape(TOTAL, 1)
    masked = jnp.where(live, foot_offset, -1)
    dma = pltpu.SemaphoreType.DMA
    vmem = pl.BlockSpec(memory_space=pltpu.VMEM)
    hbm = pl.BlockSpec(memory_space=pl.ANY)
    residual, summed, columns = pl.pallas_call(
        kernel,
        out_shape=(
            jax.ShapeDtypeStruct((YS, NCB * RB, CB), F32),
            jax.ShapeDtypeStruct((YS, SLOTS, SUB), F32),
            jax.ShapeDtypeStruct((8, TV), F32),
        ),
        in_specs=[vmem] * 5,
        out_specs=(hbm, hbm, vmem),
        scratch_shapes=[
            pltpu.VMEM((YS, SLOTS, SUB), BF16),
            pltpu.VMEM((YS, ZS * CS, SLOTS, SUB), BF16),
            pltpu.VMEM((YS, TV, TV), BF16),
            pltpu.VMEM((YS, 8, TV), F32),
            pltpu.VMEM((ZS * CS, 8, TV), F32),
            pltpu.VMEM((8, NCB * CB), BF16),
            pltpu.VMEM((8, NCB * CB), BF16),
            pltpu.VMEM((NCB, ROWS_HERE + 16, CB), F32),
            pltpu.VMEM((NCB + 2, ROWS_HERE, CB), F32),
            pltpu.VMEM((YS, NCB * RB, CB), F32),
            pltpu.VMEM((YS, NCB * RB, CB), F32),
            pltpu.VMEM((YS * BP, TOTAL), BF16),
            pltpu.VMEM((TOTAL, YS * CB), BF16),
            pltpu.VMEM((YS, RB * BP, TV), BF16),
            pltpu.VMEM((RB * BP, TV), BF16),
            pltpu.VMEM((YS, NCB * RB, CB), F32),
            pltpu.VMEM((2, YS * CB, SUB), BF16),
            pltpu.VMEM((YS, ZS, CS, SLOTS, SUB), F32),
            pltpu.VMEM((ZS, YS, SLOTS, SUB), F32),
            pltpu.VMEM((2, 4, 2, 2, SLOTS, SUB), F32),
            dma((6, 3)), dma((6, 3)),
            dma((2,)), dma((2,)),
            dma((2, 4, 3)), dma((2, 4, 3)),
            dma((8, 3)), dma((8, 3)),
            dma((8,)), dma((8,)),
            dma((2, 4, 2)), dma((2, 4, 2)),
            dma((2,)),
        ],
        compiler_params=pltpu.CompilerParams(
            collective_id=0, has_side_effects=True, vmem_limit_bytes=60 << 20
        ),
        name="sirt",
    )(intensity, volume, footprint, masked, masked.T)
    residual = (
        residual.reshape(YS, NCB, RB, CB).transpose(0, 2, 1, 3).reshape(1, ROWS_HERE, NCB * CB)
    )
    summed = summed.reshape(YS, SLOTS, RB, TV).transpose(1, 0, 2, 3).reshape(SLOTS, ROWS_HERE, TV)
    return residual, summed / columns[0][None, None, :]


def solution(mesh):
    placed = (P("tile", "row", None), P("tile", "row", None), P("tile", None, None), P(), P())
    return jax.shard_map(
        local,
        mesh=mesh,
        in_specs=placed,
        out_specs=(P("tile", "row", None), P("tile", "row", None)),
        check_vma=False,
    )
```

```python
import functools

import jax
import jax.numpy as jnp
import numpy as np
from jax import lax
from jax.experimental import pallas as pl
from jax.experimental.pallas import tpu as pltpu
from jax.sharding import PartitionSpec as P

RIM = 3
NCB = 88
CB = 128
TV = 256
YS, ZS, CS, XS = 4, 8, 2, 4
SLOTS = 8
RB = 8
SUB = RB * TV
TOTAL = YS * ZS * CS * SLOTS
BP = 96
PART = TV // XS
ROWS_HERE = YS * RB

decay_length = 2.0
row_floor = 0.5

F32 = jnp.float32
BF16 = jnp.bfloat16
MESH = pl.DeviceIdType.MESH


def smoothing_taps():
    spread_taps = np.exp(-np.abs(np.arange(-RIM, RIM + 1)) / decay_length)
    return [float(t) for t in (spread_taps / spread_taps.sum()).astype(np.float32)]


def dot(a, b, dims=((1,), (0,))):
    return lax.dot_general(a, b, (dims, ((), ())), preferred_element_type=F32)


def kernel(
    inten_h, vol, foot, off_t, count,
    res_out, cor_out, col_out,
    inten, vol_s, vol_g, foot_g, cs_y, cs_g,
    halo_lo, halo_hi, rows_p, rows_a, ph_s, ph,
    hot, hot_t, loads, images, weigh, res_w, back, terms, pair_r, ring_r, fin,
    y_send, y_recv, h_send, h_recv, x_send, x_recv, g_send, g_recv, c_send, c_recv,
    q_send, q_recv, p_send, p_recv, r_send, r_recv, f_send, f_recv, l_sem,
):
    taps = smoothing_taps()
    t = lax.axis_index("tile")
    x = lax.axis_index("row")
    y = t // (ZS * CS)
    zc = t % (ZS * CS)
    z = zc // CS
    c = zc % CS

    def tile_of(yy, zz, cc):
        return (yy * ZS + zz) * CS + cc

    def device(yy, zz, cc):
        return (tile_of(yy, zz, cc), x)

    z_up, z_down = (z + 1) % ZS, (z + ZS - 1) % ZS
    z_next = (z_up, z_down)
    partner = device(y, z, 1 - c)
    toward = (device(y, z_up, c), device(y, z_down, c))
    y_to = [(y + d) % YS for d in range(YS)]
    y_from = [(y + YS - d) % YS for d in range(YS)]
    x_to = [(x + d) % XS for d in range(XS)]
    x_from = [(x + XS - d) % XS for d in range(XS)]

    load_inten = pltpu.make_async_copy(inten_h, inten, l_sem.at[2])
    load_inten.start()

    barrier = pltpu.get_barrier_semaphore()
    peers = [device(y_to[d], z, c) for d in range(1, YS)]
    peers += [device(y_to[d], zz, c) for d in range(YS) for zz in z_next]
    peers += [(t, x_to[d]) for d in range(1, XS)] + [partner]
    for peer in peers:
        pl.semaphore_signal(barrier, inc=1, device_id=peer, device_id_type=MESH)

    for q in range(YS):
        for r in range(RB):
            vol_s[q, :, r * TV : (r + 1) * TV] = vol[:, q * RB + r, :].astype(BF16)
    pl.semaphore_wait(barrier, len(peers))

    started = []

    def send(src, dst, ssem, rsem, dev):
        copy = pltpu.make_async_remote_copy(
            src_ref=src, dst_ref=dst, send_sem=ssem, recv_sem=rsem,
            device_id=dev, device_id_type=MESH,
        )
        copy.start()
        started.append(copy)

    def arrive(dst, ssem, rsem, dev):
        pltpu.make_async_remote_copy(
            src_ref=dst, dst_ref=dst, send_sem=ssem, recv_sem=rsem,
            device_id=dev, device_id_type=MESH,
        ).wait_recv()

    def y_copy(kind, d, src, dst):
        send(src, dst, y_send.at[kind, d], y_recv.at[kind, d], device(y_to[d], z, c))

    def y_wait(kind, d, dst):
        arrive(dst, y_send.at[kind, d], y_recv.at[kind, d], device(y_from[d], z, c))

    for d in range(YS):
        for way in range(2):
            send(
                vol_s.at[y_to[d]], vol_g.at[y, zc], g_send.at[way, 0, d], g_recv.at[way, 0, d],
                device(y_to[d], z_next[way], c),
            )
    for d in range(1, YS):
        y_copy(0, d, vol_s.at[y_to[d]], vol_g.at[y, zc])
    send(inten_h.at[0, pl.ds(ROWS_HERE - 8, 8), :], halo_lo, h_send.at[0], h_recv.at[0], (t, x_to[1]))
    send(inten_h.at[0, pl.ds(0, 8), :], halo_hi, h_send.at[1], h_recv.at[1], (t, x_from[1]))
    ones = jnp.ones((8, TV), BF16)
    cs_y[y] = dot(ones, foot[0], ((1,), (1,)))
    for d in range(1, YS):
        y_copy(1, d, cs_y.at[y], cs_y.at[y])
    part = pl.ds(pl.multiple_of(x * PART, PART), PART)
    for d in range(1, YS):
        y_copy(2, d, foot.at[0, part], foot_g.at[y, part])
    vol_g[y, zc] = vol_s[y]
    foot_g[y] = foot[0]

    groups = YS * ZS * CS
    member = lax.broadcasted_iota(jnp.int32, (groups, TOTAL), 1)
    owner = lax.broadcasted_iota(jnp.int32, (groups, TOTAL), 0)
    expand = (member // SLOTS == owner).astype(F32).astype(BF16)
    counts = jnp.broadcast_to(count[...].astype(F32), (8, groups)).astype(BF16)
    slot = lax.broadcasted_iota(jnp.int32, (1, TOTAL), 1) % SLOTS
    live = slot.astype(F32) < dot(counts, expand)[0:1]
    block = lax.broadcasted_iota(jnp.int32, (BP, TOTAL), 0)
    offsets = []
    for i in range(YS):
        row = jnp.where(live, off_t[pl.ds(tile_of(i, z, c), 1), :], -1)
        hot[i * BP : (i + 1) * BP, :] = (row == block).astype(F32).astype(BF16)
        offsets.append(row.astype(F32))

    def one_hot_columns():
        rows8 = jnp.concatenate(offsets + [jnp.zeros((8 - YS, TOTAL), F32)], axis=0)
        columns = rows8.T
        block_t = lax.broadcasted_iota(jnp.int32, (TOTAL, CB), 1).astype(F32)
        for i in range(YS):
            hot_t[:, i * CB : (i + 1) * CB] = (columns[:, i : i + 1] == block_t).astype(F32).astype(BF16)
        for h in range(2):
            for i in range(YS):
                back[h, i * CB + BP : (i + 1) * CB, :] = jnp.zeros((CB - BP, SUB), BF16)

    has_lo = (x > 0).astype(F32)
    has_hi = (x < XS - 1).astype(F32)
    lane = lax.broadcasted_iota(jnp.int32, (ROWS_HERE, CB), 1)

    def vertical(b, _):
        cols = pl.ds(pl.multiple_of(b * CB, CB), CB)
        rows_p[b, 0:8, :] = halo_lo[:, cols].astype(F32) * has_lo
        rows_p[b, 8 : 8 + ROWS_HERE, :] = inten[0, :, cols].astype(F32)
        rows_p[b, 8 + ROWS_HERE : 16 + ROWS_HERE, :] = halo_hi[:, cols].astype(F32) * has_hi
        across = taps[RIM] * rows_p[b, 8 : 8 + ROWS_HERE, :]
        for k in range(1, RIM + 1):
            across = across + taps[RIM + k] * (
                rows_p[b, 8 - k : 8 - k + ROWS_HERE, :] + rows_p[b, 8 + k : 8 + k + ROWS_HERE, :]
            )
        rows_a[b + 1] = across
        return 0

    def horizontal(b, _):
        before, here, after = rows_a[b], rows_a[b + 1], rows_a[b + 2]
        smooth = taps[RIM] * here
        for k in range(1, RIM + 1):
            ahead = pltpu.roll(jnp.where(lane < k, after, here), CB - k, 1)
            behind = pltpu.roll(jnp.where(lane >= CB - k, before, here), k, 1)
            smooth = smooth + taps[RIM + k] * (ahead + behind)
        phase = -jnp.log(smooth)
        for q in range(YS):
            ph_s[q, pl.ds(pl.multiple_of(b * RB, RB), RB), :] = phase[q * RB : (q + 1) * RB]
        return 0

    quarter = NCB // 4

    def phase_part(k):
        lax.fori_loop(k * quarter, (k + 1) * quarter, horizontal, 0, unroll=2)
        span = pl.ds(k * quarter * RB, quarter * RB)
        for d in range(1, YS):
            y_copy(6 + k, d, ph_s.at[y_to[d], span], ph.at[y, span])

    def piece(d, zz):
        return vol_g.at[y_from[d], zz * CS + c]

    def give_partner(index, zz):
        src = vol_g.at[:, zz * CS + c]
        send(src, src, q_send.at[index, 0], q_recv.at[index, 0], partner)
        src = cs_g.at[zz * CS + c]
        send(src, src, q_send.at[index, 1], q_recv.at[index, 1], partner)

    def z_far(way, step):
        return (z + ZS - step) % ZS if way == 0 else (z + step) % ZS

    def sums_send(way, step, zz):
        src = cs_g.at[zz * CS + c]
        send(src, src, c_send.at[way, step], c_recv.at[way, step], toward[way])

    def serve(step):
        for d in range(YS):
            for way in range(2):
                if step == 4 and way != d // 2:
                    continue
                zz = z_far(way, step)
                here = piece(d, zz)
                arrive(here, g_send.at[way, step - 1, d], g_recv.at[way, step - 1, d], toward[1 - way])
                if step < 3 or (step == 3 and way == d // 2):
                    send(here, here, g_send.at[way, step, d], g_recv.at[way, step, d], toward[way])
        for way in range(2):
            if step == 4 and way == 1:
                continue
            zz = z_far(way, step)
            arrive(
                cs_g.at[zz * CS + c], c_send.at[way, step - 1], c_recv.at[way, step - 1], toward[1 - way]
            )
            if step < 3 or (step == 3 and way == 0):
                sums_send(way, step, zz)
            give_partner(step if way == 0 else 4 + step, zz)

    rows_a[0] = jnp.zeros((ROWS_HERE, CB), F32)
    rows_a[NCB + 1] = jnp.zeros((ROWS_HERE, CB), F32)
    for d in range(1, YS):
        y_wait(1, d, cs_y.at[y_from[d]])
    cs_g[zc] = cs_y[0] + cs_y[1] + cs_y[2] + cs_y[3]
    for way in range(2):
        sums_send(way, 0, z)
    load_inten.wait()
    arrive(halo_lo, h_send.at[0], h_recv.at[0], (t, x_from[1]))
    arrive(halo_hi, h_send.at[1], h_recv.at[1], (t, x_to[1]))
    lax.fori_loop(0, NCB, vertical, 0, unroll=2)
    serve(1)
    phase_part(0)
    phase_part(1)
    for d in range(1, YS):
        y_wait(0, d, vol_g.at[y_from[d], zc])
    give_partner(0, z)
    for d in range(1, YS):
        y_wait(2, d, foot_g.at[y_from[d], part])
        for e in range(1, XS):
            src = foot_g.at[y_from[d], part]
            send(src, src, x_send.at[d, e], x_recv.at[d, e], (t, x_to[e]))
    phase_part(2)
    phase_part(3)
    ph[y] = ph_s[y]
    serve(2)
    one_hot_columns()
    serve(3)
    serve(4)
    for d in range(1, YS):
        for e in range(1, XS):
            theirs = pl.ds(pl.multiple_of(x_from[e] * PART, PART), PART)
            arrive(foot_g.at[y_from[d], theirs], x_send.at[d, e], x_recv.at[d, e], (t, x_from[e]))
    for index in range(8):
        zz = z_far(0, index) if index < 5 else z_far(1, index - 4)
        arrive(vol_g.at[:, zz * CS + 1 - c], q_send.at[index, 0], q_recv.at[index, 0], partner)
        arrive(cs_g.at[zz * CS + 1 - c], q_send.at[index, 1], q_recv.at[index, 1], partner)

    def load_row(r, _):
        cols = pl.ds(pl.multiple_of(r * TV, TV), TV)
        got = dot(hot[...], vol_g[:, :, :, cols].reshape(TOTAL, TV)).astype(BF16)
        for i in range(YS):
            loads[i, pl.ds(pl.multiple_of(r * BP, BP), BP), :] = got[i * BP : (i + 1) * BP]
        return 0

    lax.fori_loop(0, RB, load_row, 0)

    def image(i, _):
        images[i] = dot(loads[i], foot_g[i])
        return 0

    lax.fori_loop(0, YS, image, 0)
    for k in range(4):
        span = pl.ds(k * quarter * RB, quarter * RB)
        for d in range(1, YS):
            y_wait(6 + k, d, ph.at[y_from[d], span])

    def one_angle(i, _):
        table = foot_g[i]
        counted = jnp.sum(hot[pl.ds(pl.multiple_of(i * BP, BP), BP), :].astype(F32), axis=1, keepdims=True)
        sums = dot(ones, table)[0:1]
        totals = counted * sums[:, :CB] + pltpu.roll(counted * sums[:, CB:], 1, 0)
        scale = (1.0 / jnp.maximum(totals, row_floor))[:NCB]
        for r in range(RB):
            own = images[i, r * BP : (r + 1) * BP, :]
            shadow = own[:, :CB] + pltpu.roll(own[:, CB:], 1, 0)
            left_over = ph[i, pl.ds(r, NCB, stride=RB), :] - shadow[:NCB]
            res_w[i, pl.ds(r, NCB, stride=RB), :] = left_over
            near = jnp.concatenate([left_over * scale, jnp.zeros((BP - NCB, CB), F32)], axis=0)
            far = pltpu.roll(near, BP - 1, 0)
            weigh[r * BP : (r + 1) * BP, :] = jnp.concatenate([near, far], axis=1).astype(BF16)
        spread = dot(weigh[...], table, ((1,), (1,)))
        rows = pl.ds(pl.multiple_of(i * CB, CB), BP)
        for r in range(RB):
            given = spread[r * BP : (r + 1) * BP]
            high = given.astype(BF16)
            back[0, rows, r * TV : (r + 1) * TV] = high
            back[1, rows, r * TV : (r + 1) * TV] = (given - high.astype(F32)).astype(BF16)
        return 0

    lax.fori_loop(0, YS, one_angle, 0)
    for d in range(1, YS):
        y_copy(3, d, res_w.at[y_to[d]], res_out.at[y])
    own_res = pltpu.make_async_copy(res_w.at[y], res_out.at[y], l_sem.at[0])
    own_res.start()

    def term_row(r, _):
        cols = pl.ds(pl.multiple_of(r * TV, TV), TV)
        got = dot(hot_t[...], back[0, :, cols]) + dot(hot_t[...], back[1, :, cols])
        terms[:, :, :, :, cols] = got.reshape(YS, ZS, CS, SLOTS, TV)
        return 0

    halves = [pl.ds(0, SUB // 2), pl.ds(SUB // 2, SUB // 2)]
    for p in range(2):
        lax.fori_loop(p * RB // 2, (p + 1) * RB // 2, term_row, 0)
        for off in (4, 3, 5, 2, 6, 1, 7, 0):
            zz = (z + off) % ZS
            send(
                terms.at[:, zz, 1 - c, :, halves[p]], pair_r.at[zz, :, :, halves[p]],
                p_send.at[off, p], p_recv.at[off, p], partner,
            )

    def add_pair(off, p):
        zz = (z + off) % ZS
        half = halves[p]
        arrive(pair_r.at[zz, :, :, half], p_send.at[off, p], p_recv.at[off, p], partner)
        terms[:, zz, c, :, half] = terms[:, zz, c, :, half] + pair_r[zz, :, :, half]

    for step in range(4):
        for p in range(2):
            for way in range(2):
                off = 4 - step if way == 0 else 4 + step
                half = halves[p]
                if step == 0 and p != way:
                    continue
                add_pair(off, p)
                zz = (z + off) % ZS
                if step > 1 or (step == 1 and p == way):
                    got = ring_r.at[way, step - 1, p]
                    arrive(got, r_send.at[way, step - 1, p], r_recv.at[way, step - 1, p], toward[1 - way])
                    terms[:, zz, c, :, half] = terms[:, zz, c, :, half] + ring_r[way, step - 1, p]
                if step < 3:
                    send(
                        terms.at[:, zz, c, :, half], ring_r.at[way, step, p],
                        r_send.at[way, step, p], r_recv.at[way, step, p], toward[way],
                    )
                    continue
                for d in range(YS):
                    send(
                        terms.at[y_to[d], zz, c, :, half], fin.at[way, y, :, half],
                        f_send.at[way, p, d], f_recv.at[way, p, d], device(y_to[d], zz, c),
                    )
        if step == 1:
            for p in range(2):
                add_pair(0, p)
            for d in range(1, YS):
                y_copy(4, d, terms.at[y_to[d], z, c], fin.at[2, y])
            fin[2, y] = terms[y, z, c]

    total = cs_g[0]
    for k in range(1, ZS * CS):
        total = total + cs_g[k]
    col_out[...] = 1.0 / total
    for d in range(1, YS):
        y_wait(3, d, res_out.at[y_from[d]])
    for d in range(1, YS):
        y_wait(4, d, fin.at[2, y_from[d]])
    for p in range(2):
        for d in range(YS):
            for way in range(2):
                arrive(
                    fin.at[way, y_from[d], :, halves[p]], f_send.at[way, p, d], f_recv.at[way, p, d],
                    device(y_from[d], z_next[1 - way], c),
                )
    for q in range(YS):
        cor_out[q] = fin[0, q] + fin[1, q] + fin[2, q]
    own_res.wait()
    for copy in started:
        copy.wait_send()


def finish(res, cor, col, res_out, cor_out):
    for b in range(NCB):
        res_out[0, :, b * CB : (b + 1) * CB] = res[0, b * RB : (b + 1) * RB, :]
    for r in range(RB):
        cor_out[:, r, :] = cor[0, :, r * TV : (r + 1) * TV] * col[...]


def local(intensity, volume, footprint, foot_offset, tile_count):
    dma = pltpu.SemaphoreType.DMA
    vmem = pl.BlockSpec(memory_space=pltpu.VMEM)
    hbm = pl.BlockSpec(memory_space=pl.ANY)
    residual, summed, columns = pl.pallas_call(
        kernel,
        out_shape=(
            jax.ShapeDtypeStruct((YS, NCB * RB, CB), F32),
            jax.ShapeDtypeStruct((YS, SLOTS, SUB), F32),
            jax.ShapeDtypeStruct((8, TV), F32),
        ),
        in_specs=[hbm] + [vmem] * 4,
        out_specs=(hbm, vmem, vmem),
        scratch_shapes=[
            pltpu.VMEM((1, ROWS_HERE, NCB * CB), BF16),
            pltpu.VMEM((YS, SLOTS, SUB), BF16),
            pltpu.VMEM((YS, ZS * CS, SLOTS, SUB), BF16),
            pltpu.VMEM((YS, TV, TV), BF16),
            pltpu.VMEM((YS, 8, TV), F32),
            pltpu.VMEM((ZS * CS, 8, TV), F32),
            pltpu.VMEM((8, NCB * CB), BF16),
            pltpu.VMEM((8, NCB * CB), BF16),
            pltpu.VMEM((NCB, ROWS_HERE + 16, CB), F32),
            pltpu.VMEM((NCB + 2, ROWS_HERE, CB), F32),
            pltpu.VMEM((YS, NCB * RB, CB), F32),
            pltpu.VMEM((YS, NCB * RB, CB), F32),
            pltpu.VMEM((YS * BP, TOTAL), BF16),
            pltpu.VMEM((TOTAL, YS * CB), BF16),
            pltpu.VMEM((YS, RB * BP, TV), BF16),
            pltpu.VMEM((YS, RB * BP, TV), F32),
            pltpu.VMEM((RB * BP, TV), BF16),
            pltpu.VMEM((YS, NCB * RB, CB), F32),
            pltpu.VMEM((2, YS * CB, SUB), BF16),
            pltpu.VMEM((YS, ZS, CS, SLOTS, SUB), F32),
            pltpu.VMEM((ZS, YS, SLOTS, SUB), F32),
            pltpu.VMEM((2, 3, 2, YS, SLOTS, SUB // 2), F32),
            pltpu.VMEM((3, YS, SLOTS, SUB), F32),
            dma((10, 4)), dma((10, 4)),
            dma((2,)), dma((2,)),
            dma((4, 4)), dma((4, 4)),
            dma((2, 4, 4)), dma((2, 4, 4)),
            dma((2, 4)), dma((2, 4)),
            dma((8, 2)), dma((8, 2)),
            dma((8, 2)), dma((8, 2)),
            dma((2, 3, 2)), dma((2, 3, 2)),
            dma((2, 2, 4)), dma((2, 2, 4)),
            dma((3,)),
        ],
        compiler_params=pltpu.CompilerParams(
            collective_id=0, has_side_effects=True, vmem_limit_bytes=60 << 20
        ),
        name="sirt",
    )(intensity, volume, footprint, foot_offset.T, tile_count.reshape(1, -1))
    return pl.pallas_call(
        finish,
        grid=(YS,),
        out_shape=(
            jax.ShapeDtypeStruct((1, ROWS_HERE, NCB * CB), F32),
            jax.ShapeDtypeStruct((SLOTS, ROWS_HERE, TV), F32),
        ),
        in_specs=[
            pl.BlockSpec((1, NCB * RB, CB), lambda q: (q, 0, 0)),
            pl.BlockSpec((1, SLOTS, SUB), lambda q: (q, 0, 0)),
            pl.BlockSpec((8, TV), lambda q: (0, 0)),
        ],
        out_specs=(
            pl.BlockSpec((1, RB, NCB * CB), lambda q: (0, q, 0)),
            pl.BlockSpec((SLOTS, RB, TV), lambda q: (0, q, 0)),
        ),
        name="finish",
    )(residual, summed, columns)


def solution(mesh):
    placed = (P("tile", "row", None), P("tile", "row", None), P("tile", None, None), P(), P())
    return jax.shard_map(
        local,
        mesh=mesh,
        in_specs=placed,
        out_specs=(P("tile", "row", None), P("tile", "row", None)),
        check_vma=False,
    )
```

```python
import functools

import jax
import jax.numpy as jnp
import numpy as np
from jax import lax
from jax.experimental import pallas as pl
from jax.experimental.pallas import tpu as pltpu
from jax.sharding import PartitionSpec as P

RIM = 3
NCB = 88
CB = 128
TV = 256
YS, ZS, CS, XS = 4, 8, 2, 4
SLOTS = 8
RB = 8
SUB = RB * TV
TOTAL = YS * ZS * CS * SLOTS
BP = 96
PART = TV // XS
HB = RB // 2
HR = NCB * HB
HS = HB * TV
ROWS_HERE = YS * RB

decay_length = 2.0
row_floor = 0.5

F32 = jnp.float32
BF16 = jnp.bfloat16
MESH = pl.DeviceIdType.MESH


def smoothing_taps():
    spread_taps = np.exp(-np.abs(np.arange(-RIM, RIM + 1)) / decay_length)
    return [float(t) for t in (spread_taps / spread_taps.sum()).astype(np.float32)]


def dot(a, b, dims=((1,), (0,))):
    return lax.dot_general(a, b, (dims, ((), ())), preferred_element_type=F32)


def kernel(
    inten_h, vol, foot, off_t, count,
    res_out, cor_out, col_out,
    inten, vol_s, vol_g, foot_g, cs_y, cs_g,
    halo_lo, halo_hi, rows_p, rows_a, ph_s, ph,
    hot, hot_t, loads, images, scale_s, weigh, res_w, back, terms, pair_r, ring_r, fin,
    y_send, y_recv, h_send, h_recv, x_send, x_recv, g_send, g_recv, c_send, c_recv,
    q_send, q_recv, p_send, p_recv, r_send, r_recv, l_sem,
):
    taps = smoothing_taps()
    t = lax.axis_index("tile")
    x = lax.axis_index("row")
    y = t // (ZS * CS)
    zc = t % (ZS * CS)
    z = zc // CS
    c = zc % CS

    def tile_of(yy, zz, cc):
        return (yy * ZS + zz) * CS + cc

    def device(yy, zz, cc):
        return (tile_of(yy, zz, cc), x)

    z_up, z_down = (z + 1) % ZS, (z + ZS - 1) % ZS
    partner = device(y, z, 1 - c)
    toward = (device(y, z_up, c), device(y, z_down, c))
    y_to = [(y + d) % YS for d in range(YS)]
    y_from = [(y + YS - d) % YS for d in range(YS)]
    x_to = [(x + d) % XS for d in range(XS)]
    x_from = [(x + XS - d) % XS for d in range(XS)]

    load_inten = pltpu.make_async_copy(inten_h, inten, l_sem.at[2])
    load_inten.start()

    barrier = pltpu.get_barrier_semaphore()
    peers = [device(y_to[d], z, c) for d in range(1, YS)]
    peers += [device(y, zz, c) for zz in (z_up, z_down)]
    peers += [(t, x_to[d]) for d in range(1, XS)] + [partner]
    for peer in peers:
        pl.semaphore_signal(barrier, inc=1, device_id=peer, device_id_type=MESH)

    for q in range(YS):
        for r in range(RB):
            vol_s[q, :, r * TV : (r + 1) * TV] = vol[:, q * RB + r, :].astype(BF16)
    pl.semaphore_wait(barrier, len(peers))

    started = []

    def send(src, dst, ssem, rsem, dev):
        copy = pltpu.make_async_remote_copy(
            src_ref=src, dst_ref=dst, send_sem=ssem, recv_sem=rsem,
            device_id=dev, device_id_type=MESH,
        )
        copy.start()
        started.append(copy)

    def arrive(dst, ssem, rsem, dev):
        pltpu.make_async_remote_copy(
            src_ref=dst, dst_ref=dst, send_sem=ssem, recv_sem=rsem,
            device_id=dev, device_id_type=MESH,
        ).wait_recv()

    def y_copy(kind, d, src, dst):
        send(src, dst, y_send.at[kind, d], y_recv.at[kind, d], device(y_to[d], z, c))

    def y_wait(kind, d, dst):
        arrive(dst, y_send.at[kind, d], y_recv.at[kind, d], device(y_from[d], z, c))

    halves = [pl.ds(0, HS), pl.ds(HS, HS)]

    for h in range(2):
        for d in range(1, YS):
            y_copy(h, d, vol_s.at[y_to[d], :, halves[h]], vol_g.at[y, zc, :, halves[h]])
    quarter = NCB // 4
    load_inten.wait()
    for k in range(4):
        cols = pl.ds(k * quarter * CB, quarter * CB)
        send(
            inten.at[0, pl.ds(ROWS_HERE - 8, 8), cols], halo_lo.at[:, cols],
            h_send.at[0, k], h_recv.at[0, k], (t, x_to[1]),
        )
        send(inten.at[0, pl.ds(0, 8), cols], halo_hi.at[:, cols], h_send.at[1, k], h_recv.at[1, k], (t, x_from[1]))
    ones = jnp.ones((8, TV), BF16)
    cs_y[y] = dot(ones, foot[0], ((1,), (1,)))
    for d in range(1, YS):
        y_copy(2, d, cs_y.at[y], cs_y.at[y])
    part = pl.ds(pl.multiple_of(x * PART, PART), PART)
    for d in range(1, YS):
        y_copy(3, d, foot.at[0, part], foot_g.at[y, part])
    vol_g[y, zc] = vol_s[y]
    foot_g[y] = foot[0]

    groups = YS * ZS * CS
    member = lax.broadcasted_iota(jnp.int32, (groups, TOTAL), 1)
    owner = lax.broadcasted_iota(jnp.int32, (groups, TOTAL), 0)
    expand = (member // SLOTS == owner).astype(F32).astype(BF16)
    counts = jnp.broadcast_to(count[...].astype(F32), (8, groups)).astype(BF16)
    slot = lax.broadcasted_iota(jnp.int32, (1, TOTAL), 1) % SLOTS
    live = slot.astype(F32) < dot(counts, expand)[0:1]
    block = lax.broadcasted_iota(jnp.int32, (BP, TOTAL), 0)
    offsets = []
    for i in range(YS):
        row = jnp.where(live, off_t[pl.ds(tile_of(i, z, c), 1), :], -1)
        hot[i * BP : (i + 1) * BP, :] = (row == block).astype(F32).astype(BF16)
        offsets.append(row.astype(F32))

    def one_hot_columns():
        rows8 = jnp.concatenate(offsets + [jnp.zeros((8 - YS, TOTAL), F32)], axis=0)
        columns = rows8.T
        block_t = lax.broadcasted_iota(jnp.int32, (TOTAL, CB), 1).astype(F32)
        for i in range(YS):
            hot_t[:, i * CB : (i + 1) * CB] = (columns[:, i : i + 1] == block_t).astype(F32).astype(BF16)
        for h in range(2):
            for i in range(YS):
                back[h, i * CB + BP : (i + 1) * CB, :] = jnp.zeros((CB - BP, SUB), BF16)

    has_lo = (x > 0).astype(F32)
    has_hi = (x < XS - 1).astype(F32)
    lane = lax.broadcasted_iota(jnp.int32, (ROWS_HERE, CB), 1)

    def vertical(b, _):
        cols = pl.ds(pl.multiple_of(b * CB, CB), CB)
        rows_p[b, 0:8, :] = halo_lo[:, cols].astype(F32) * has_lo
        rows_p[b, 8 : 8 + ROWS_HERE, :] = inten[0, :, cols].astype(F32)
        rows_p[b, 8 + ROWS_HERE : 16 + ROWS_HERE, :] = halo_hi[:, cols].astype(F32) * has_hi
        across = taps[RIM] * rows_p[b, 8 : 8 + ROWS_HERE, :]
        for k in range(1, RIM + 1):
            across = across + taps[RIM + k] * (
                rows_p[b, 8 - k : 8 - k + ROWS_HERE, :] + rows_p[b, 8 + k : 8 + k + ROWS_HERE, :]
            )
        rows_a[b + 1] = across
        return 0

    def horizontal(b, _):
        before, here, after = rows_a[b], rows_a[b + 1], rows_a[b + 2]
        smooth = taps[RIM] * here
        for k in range(1, RIM + 1):
            ahead = pltpu.roll(jnp.where(lane < k, after, here), CB - k, 1)
            behind = pltpu.roll(jnp.where(lane >= CB - k, before, here), k, 1)
            smooth = smooth + taps[RIM + k] * (ahead + behind)
        phase = -jnp.log(smooth)
        for q in range(YS):
            for h in range(2):
                first = q * RB + h * HB
                ph_s[q, h, pl.ds(pl.multiple_of(b * HB, HB), HB), :] = phase[first : first + HB]
        return 0

    def smooth_rows(k):
        cols = pl.ds(k * quarter * CB, quarter * CB)
        arrive(halo_lo.at[:, cols], h_send.at[0, k], h_recv.at[0, k], (t, x_from[1]))
        arrive(halo_hi.at[:, cols], h_send.at[1, k], h_recv.at[1, k], (t, x_to[1]))
        lax.fori_loop(k * quarter, (k + 1) * quarter, vertical, 0, unroll=2)

    def phase_part(k):
        lax.fori_loop(k * quarter, (k + 1) * quarter, horizontal, 0, unroll=2)
        span = pl.ds(k * quarter * HB, quarter * HB)
        for d in range(1, YS):
            y_copy(6 + k, d, ph_s.at[y_to[d], 0, span], ph.at[y, 0, span])

    def piece(h, zz, cc):
        return vol_g.at[:, zz * CS + cc, :, halves[h]]

    def give_partner(index, zz, h):
        src = piece(h, zz, c)
        send(src, src, q_send.at[index, h], q_recv.at[index, h], partner)

    def give_partner_sums(index, zz):
        src = cs_g.at[zz * CS + c]
        send(src, src, q_send.at[index, 2], q_recv.at[index, 2], partner)

    def ring_send(way, step, h, zz):
        src = piece(h, zz, c)
        send(src, src, g_send.at[way, step, h], g_recv.at[way, step, h], toward[way])

    def z_far(way, step):
        return (z + ZS - step) % ZS if way == 0 else (z + step) % ZS

    def sums_send(way, step, zz):
        src = cs_g.at[zz * CS + c]
        send(src, src, c_send.at[way, step], c_recv.at[way, step], toward[way])

    def serve(step):
        for h in range(2):
            for way in range(2):
                if step == 4 and way != h:
                    continue
                zz = z_far(way, step)
                arrive(
                    piece(h, zz, c), g_send.at[way, step - 1, h], g_recv.at[way, step - 1, h],
                    toward[1 - way],
                )
                if step < 3 or (step == 3 and way == h):
                    ring_send(way, step, h, zz)
                give_partner(step if way == 0 or step == 4 else 4 + step, zz, h)
        for way in range(2):
            if step == 4 and way == 1:
                continue
            zz = z_far(way, step)
            arrive(
                cs_g.at[zz * CS + c], c_send.at[way, step - 1], c_recv.at[way, step - 1], toward[1 - way]
            )
            if step < 3 or (step == 3 and way == 0):
                sums_send(way, step, zz)
            give_partner_sums(step if way == 0 else 4 + step, zz)

    rows_a[0] = jnp.zeros((ROWS_HERE, CB), F32)
    rows_a[NCB + 1] = jnp.zeros((ROWS_HERE, CB), F32)
    for h in range(2):
        for d in range(1, YS):
            y_wait(h, d, vol_g.at[y_from[d], zc, :, halves[h]])
        for way in range(2):
            ring_send(way, 0, h, z)
        give_partner(0, z, h)
    for d in range(1, YS):
        y_wait(2, d, cs_y.at[y_from[d]])
    cs_g[zc] = cs_y[0] + cs_y[1] + cs_y[2] + cs_y[3]
    for way in range(2):
        sums_send(way, 0, z)
    give_partner_sums(0, z)
    smooth_rows(0)
    smooth_rows(1)
    phase_part(0)
    serve(1)
    smooth_rows(2)
    phase_part(1)
    smooth_rows(3)
    phase_part(2)
    serve(2)
    phase_part(3)
    for d in range(1, YS):
        y_copy(4, d, ph_s.at[y_to[d], 1], ph.at[y, 1])
    ph[y] = ph_s[y]
    for d in range(1, YS):
        y_wait(3, d, foot_g.at[y_from[d], part])
        for e in range(1, XS):
            src = foot_g.at[y_from[d], part]
            send(src, src, x_send.at[d, e], x_recv.at[d, e], (t, x_to[e]))
    serve(3)
    one_hot_columns()
    for d in range(1, YS):
        for e in range(1, XS):
            theirs = pl.ds(pl.multiple_of(x_from[e] * PART, PART), PART)
            arrive(foot_g.at[y_from[d], theirs], x_send.at[d, e], x_recv.at[d, e], (t, x_from[e]))
    serve(4)

    def take_partner(h):
        for index in range(8):
            zz = z_far(0, index) if index < 5 else z_far(1, index - 4)
            arrive(piece(h, zz, 1 - c), q_send.at[index, h], q_recv.at[index, h], partner)
            if h == 1:
                arrive(cs_g.at[zz * CS + 1 - c], q_send.at[index, 2], q_recv.at[index, 2], partner)

    def scales(i, _):
        counted = jnp.sum(hot[pl.ds(pl.multiple_of(i * BP, BP), BP), :].astype(F32), axis=1, keepdims=True)
        sums = dot(ones, foot_g[i])[0:1]
        totals = counted * sums[:, :CB] + pltpu.roll(counted * sums[:, CB:], 1, 0)
        scale_s[i] = 1.0 / jnp.maximum(totals, row_floor)
        return 0

    lax.fori_loop(0, YS, scales, 0)

    def shadows(h):
        take_partner(h)

        def load_row(r, _):
            cols = pl.ds(pl.multiple_of((h * HB + r) * TV, TV), TV)
            got = dot(hot[...], vol_g[:, :, :, cols].reshape(TOTAL, TV)).astype(BF16)
            for i in range(YS):
                loads[i, pl.ds(pl.multiple_of(r * BP, BP), BP), :] = got[i * BP : (i + 1) * BP]
            return 0

        lax.fori_loop(0, HB, load_row, 0)

        def image(i, _):
            images[h, i] = dot(loads[i], foot_g[i])
            return 0

        lax.fori_loop(0, YS, image, 0)

    def weights(h):
        if h == 0:
            for k in range(4):
                span = pl.ds(k * quarter * HB, quarter * HB)
                for d in range(1, YS):
                    y_wait(6 + k, d, ph.at[y_from[d], 0, span])
        else:
            for d in range(1, YS):
                y_wait(4, d, ph.at[y_from[d], 1])

        def one_angle(i, _):
            scale = scale_s[i, :NCB, :]
            for r in range(HB):
                own = images[h, i, r * BP : (r + 1) * BP, :]
                shadow = own[:, :CB] + pltpu.roll(own[:, CB:], 1, 0)
                left_over = ph[i, h, pl.ds(r, NCB, stride=HB), :] - shadow[:NCB]
                res_w[i, h, pl.ds(r, NCB, stride=HB), :] = left_over
                near = jnp.concatenate([left_over * scale, jnp.zeros((BP - NCB, CB), F32)], axis=0)
                far = pltpu.roll(near, BP - 1, 0)
                weigh[r * BP : (r + 1) * BP, :] = jnp.concatenate([near, far], axis=1).astype(BF16)
            spread = dot(weigh[...], foot_g[i], ((1,), (1,)))
            rows = pl.ds(pl.multiple_of(i * CB, CB), BP)
            for r in range(HB):
                given = spread[r * BP : (r + 1) * BP]
                high = given.astype(BF16)
                cols = pl.ds((h * HB + r) * TV, TV)
                back[0, rows, cols] = high
                back[1, rows, cols] = (given - high.astype(F32)).astype(BF16)
            return 0

        lax.fori_loop(0, YS, one_angle, 0)
        for d in range(1, YS):
            y_copy(10 + h, d, res_w.at[y_to[d], h], res_out.at[y, h])
        pltpu.make_async_copy(res_w.at[y, h], res_out.at[y, h], l_sem.at[h]).start()

    def sums_of(h):
        def term_row(r, _):
            cols = pl.ds(pl.multiple_of(r * TV, TV), TV)
            got = dot(hot_t[...], back[0, :, cols]) + dot(hot_t[...], back[1, :, cols])
            terms[:, :, :, :, cols] = got.reshape(YS, ZS, CS, SLOTS, TV)
            return 0

        lax.fori_loop(h * HB, (h + 1) * HB, term_row, 0)
        for off in (4, 3, 5, 2, 6, 1, 7, 0):
            zz = (z + off) % ZS
            send(
                terms.at[:, zz, 1 - c, :, halves[h]], pair_r.at[h, zz],
                p_send.at[off, h], p_recv.at[off, h], partner,
            )

    def add_pair(off, h):
        zz = (z + off) % ZS
        arrive(pair_r.at[h, zz], p_send.at[off, h], p_recv.at[off, h], partner)
        terms[:, zz, c, :, halves[h]] = terms[:, zz, c, :, halves[h]] + pair_r[h, zz]

    def add_ring(way, step, h, p, zz):
        got = ring_r.at[h, way, step, p]
        arrive(got, r_send.at[h, way, step, p], r_recv.at[h, way, step, p], toward[1 - way])
        ys = pl.ds(2 * p, 2)
        terms[ys, zz, c, :, halves[h]] = terms[ys, zz, c, :, halves[h]] + ring_r[h, way, step, p]

    def sum_step(h, step):
        for way in range(2):
            if step > 0 or way == 0:
                add_pair(4 - step if way == 0 else 4 + step, h)
        for p in range(2):
            for way in range(2):
                if step == 0 and p != way:
                    continue
                zz = (z + 4 - step) % ZS if way == 0 else (z + 4 + step) % ZS
                if step > 1 or (step == 1 and p == way):
                    add_ring(way, step - 1, h, p, zz)
                send(
                    terms.at[pl.ds(2 * p, 2), zz, c, :, halves[h]], ring_r.at[h, way, step, p],
                    r_send.at[h, way, step, p], r_recv.at[h, way, step, p], toward[way],
                )
        if step == 2:
            add_pair(0, h)

    def sum_end(h):
        for p in range(2):
            for way in range(2):
                add_ring(way, 3, h, p, z)
        for d in range(1, YS):
            y_copy(12 + h, d, terms.at[y_to[d], z, c, :, halves[h]], fin.at[h, y])
        fin[h, y] = terms[y, z, c, :, halves[h]]

    shadows(0)
    weights(0)
    sums_of(0)
    sum_step(0, 0)
    shadows(1)
    sum_step(0, 1)
    weights(1)
    sums_of(1)
    sum_step(0, 2)
    sum_step(1, 0)
    sum_step(0, 3)
    sum_step(1, 1)
    sum_step(1, 2)
    sum_end(0)
    sum_step(1, 3)
    total = cs_g[0]
    for k in range(1, ZS * CS):
        total = total + cs_g[k]
    col_out[...] = 1.0 / total
    sum_end(1)
    for h in range(2):
        for d in range(1, YS):
            y_wait(10 + h, d, res_out.at[y_from[d], h])
        for d in range(1, YS):
            y_wait(12 + h, d, fin.at[h, y_from[d]])
        cor_out[h] = fin[h]
        pltpu.make_async_copy(res_w.at[y, h], res_out.at[y, h], l_sem.at[h]).wait()
    for copy in started:
        copy.wait_send()


def finish(res, cor, col, res_out, cor_out):
    for h in range(2):
        for b in range(NCB):
            res_out[0, h * HB : (h + 1) * HB, b * CB : (b + 1) * CB] = res[0, h, b * HB : (b + 1) * HB, :]
        for r in range(HB):
            cor_out[:, h * HB + r, :] = cor[h, 0, :, r * TV : (r + 1) * TV] * col[...]


def local(intensity, volume, footprint, foot_offset, tile_count):
    dma = pltpu.SemaphoreType.DMA
    vmem = pl.BlockSpec(memory_space=pltpu.VMEM)
    hbm = pl.BlockSpec(memory_space=pl.ANY)
    residual, summed, columns = pl.pallas_call(
        kernel,
        out_shape=(
            jax.ShapeDtypeStruct((YS, 2, HR, CB), F32),
            jax.ShapeDtypeStruct((2, YS, SLOTS, HS), F32),
            jax.ShapeDtypeStruct((8, TV), F32),
        ),
        in_specs=[hbm] + [vmem] * 4,
        out_specs=(hbm, vmem, vmem),
        scratch_shapes=[
            pltpu.VMEM((1, ROWS_HERE, NCB * CB), BF16),
            pltpu.VMEM((YS, SLOTS, SUB), BF16),
            pltpu.VMEM((YS, ZS * CS, SLOTS, SUB), BF16),
            pltpu.VMEM((YS, TV, TV), BF16),
            pltpu.VMEM((YS, 8, TV), F32),
            pltpu.VMEM((ZS * CS, 8, TV), F32),
            pltpu.VMEM((8, NCB * CB), BF16),
            pltpu.VMEM((8, NCB * CB), BF16),
            pltpu.VMEM((NCB, ROWS_HERE + 16, CB), F32),
            pltpu.VMEM((NCB + 2, ROWS_HERE, CB), F32),
            pltpu.VMEM((YS, 2, HR, CB), F32),
            pltpu.VMEM((YS, 2, HR, CB), F32),
            pltpu.VMEM((YS * BP, TOTAL), BF16),
            pltpu.VMEM((TOTAL, YS * CB), BF16),
            pltpu.VMEM((YS, HB * BP, TV), BF16),
            pltpu.VMEM((2, YS, HB * BP, TV), F32),
            pltpu.VMEM((YS, BP, CB), F32),
            pltpu.VMEM((HB * BP, TV), BF16),
            pltpu.VMEM((YS, 2, HR, CB), F32),
            pltpu.VMEM((2, YS * CB, SUB), BF16),
            pltpu.VMEM((YS, ZS, CS, SLOTS, SUB), F32),
            pltpu.VMEM((2, ZS, YS, SLOTS, HS), F32),
            pltpu.VMEM((2, 2, 4, 2, 2, SLOTS, HS), F32),
            pltpu.VMEM((2, YS, SLOTS, HS), F32),
            dma((14, 4)), dma((14, 4)),
            dma((2, 4)), dma((2, 4)),
            dma((4, 4)), dma((4, 4)),
            dma((2, 4, 2)), dma((2, 4, 2)),
            dma((2, 4)), dma((2, 4)),
            dma((8, 3)), dma((8, 3)),
            dma((8, 2)), dma((8, 2)),
            dma((2, 2, 4, 2)), dma((2, 2, 4, 2)),
            dma((3,)),
        ],
        compiler_params=pltpu.CompilerParams(
            collective_id=0, has_side_effects=True, vmem_limit_bytes=60 << 20
        ),
        name="sirt",
    )(intensity, volume, footprint, foot_offset.T, tile_count.reshape(1, -1))
    return pl.pallas_call(
        finish,
        grid=(YS,),
        out_shape=(
            jax.ShapeDtypeStruct((1, ROWS_HERE, NCB * CB), F32),
            jax.ShapeDtypeStruct((SLOTS, ROWS_HERE, TV), F32),
        ),
        in_specs=[
            pl.BlockSpec((1, 2, HR, CB), lambda q: (q, 0, 0, 0)),
            pl.BlockSpec((2, 1, SLOTS, HS), lambda q: (0, q, 0, 0)),
            pl.BlockSpec((8, TV), lambda q: (0, 0)),
        ],
        out_specs=(
            pl.BlockSpec((1, RB, NCB * CB), lambda q: (0, q, 0)),
            pl.BlockSpec((SLOTS, RB, TV), lambda q: (0, q, 0)),
        ),
        name="finish",
    )(residual, summed, columns)


def solution(mesh):
    placed = (P("tile", "row", None), P("tile", "row", None), P("tile", None, None), P(), P())
    return jax.shard_map(
        local,
        mesh=mesh,
        in_specs=placed,
        out_specs=(P("tile", "row", None), P("tile", "row", None)),
        check_vma=False,
    )
```

```python
import functools

import jax
import jax.numpy as jnp
import numpy as np
from jax import lax
from jax.experimental import pallas as pl
from jax.experimental.pallas import tpu as pltpu
from jax.sharding import PartitionSpec as P

RIM = 3
NCB = 88
CB = 128
TV = 256
YS, ZS, CS, XS = 4, 8, 2, 4
SLOTS = 8
RB = 8
SUB = RB * TV
TOTAL = YS * ZS * CS * SLOTS
BP = 96
PART = TV // XS
HB = RB // 2
HR = NCB * HB
HS = HB * TV
ROWS_HERE = YS * RB

decay_length = 2.0
row_floor = 0.5

F32 = jnp.float32
BF16 = jnp.bfloat16
MESH = pl.DeviceIdType.MESH


def smoothing_taps():
    spread_taps = np.exp(-np.abs(np.arange(-RIM, RIM + 1)) / decay_length)
    return [float(t) for t in (spread_taps / spread_taps.sum()).astype(np.float32)]


def dot(a, b, dims=((1,), (0,))):
    return lax.dot_general(a, b, (dims, ((), ())), preferred_element_type=F32)


def kernel(
    inten_h, vol, foot, off_t, count,
    res_out, cor_out, col_out,
    inten, vol_s, vol_g, foot_g, cs_y, cs_g,
    halo_lo, halo_hi, rows_p, rows_a, ph_s, ph,
    hot, hot_t, loads, images, scale_s, weigh, res_w, back, terms, pair_r, ring_r, fin,
    y_send, y_recv, h_send, h_recv, x_send, x_recv, g_send, g_recv, c_send, c_recv,
    q_send, q_recv, p_send, p_recv, r_send, r_recv, l_sem,
):
    taps = smoothing_taps()
    t = lax.axis_index("tile")
    x = lax.axis_index("row")
    y = t // (ZS * CS)
    zc = t % (ZS * CS)
    z = zc // CS
    c = zc % CS

    def tile_of(yy, zz, cc):
        return (yy * ZS + zz) * CS + cc

    def device(yy, zz, cc):
        return (tile_of(yy, zz, cc), x)

    z_up, z_down = (z + 1) % ZS, (z + ZS - 1) % ZS
    partner = device(y, z, 1 - c)
    toward = (device(y, z_up, c), device(y, z_down, c))
    y_to = [(y + d) % YS for d in range(YS)]
    y_from = [(y + YS - d) % YS for d in range(YS)]
    x_to = [(x + d) % XS for d in range(XS)]
    x_from = [(x + XS - d) % XS for d in range(XS)]

    load_inten = pltpu.make_async_copy(inten_h, inten, l_sem.at[2])
    load_inten.start()

    barrier = pltpu.get_barrier_semaphore()
    peers = [device(y_to[d], z, c) for d in range(1, YS)]
    peers += [device(y, zz, c) for zz in (z_up, z_down)]
    peers += [(t, x_to[d]) for d in range(1, XS)] + [partner]
    for peer in peers:
        pl.semaphore_signal(barrier, inc=1, device_id=peer, device_id_type=MESH)

    for q in range(YS):
        for r in range(RB):
            vol_s[q, :, r * TV : (r + 1) * TV] = vol[:, q * RB + r, :].astype(BF16)
    pl.semaphore_wait(barrier, len(peers))

    started = []

    def send(src, dst, ssem, rsem, dev):
        copy = pltpu.make_async_remote_copy(
            src_ref=src, dst_ref=dst, send_sem=ssem, recv_sem=rsem,
            device_id=dev, device_id_type=MESH,
        )
        copy.start()
        started.append(copy)

    def arrive(dst, ssem, rsem, dev):
        pltpu.make_async_remote_copy(
            src_ref=dst, dst_ref=dst, send_sem=ssem, recv_sem=rsem,
            device_id=dev, device_id_type=MESH,
        ).wait_recv()

    def y_copy(kind, d, src, dst):
        send(src, dst, y_send.at[kind, d], y_recv.at[kind, d], device(y_to[d], z, c))

    def y_wait(kind, d, dst):
        arrive(dst, y_send.at[kind, d], y_recv.at[kind, d], device(y_from[d], z, c))

    halves = [pl.ds(0, HS), pl.ds(HS, HS)]

    for h in range(2):
        for d in range(1, YS):
            y_copy(h, d, vol_s.at[y_to[d], :, halves[h]], vol_g.at[y, zc, :, halves[h]])
    quarter = NCB // 4
    load_inten.wait()
    for k in range(4):
        cols = pl.ds(k * quarter * CB, quarter * CB)
        send(
            inten.at[0, pl.ds(ROWS_HERE - 8, 8), cols], halo_lo.at[:, cols],
            h_send.at[0, k], h_recv.at[0, k], (t, x_to[1]),
        )
        send(inten.at[0, pl.ds(0, 8), cols], halo_hi.at[:, cols], h_send.at[1, k], h_recv.at[1, k], (t, x_from[1]))
    ones = jnp.ones((8, TV), BF16)
    cs_y[y] = dot(ones, foot[0], ((1,), (1,)))
    for d in range(1, YS):
        y_copy(2, d, cs_y.at[y], cs_y.at[y])
    part = pl.ds(pl.multiple_of(x * PART, PART), PART)
    for d in range(1, YS):
        y_copy(3, d, foot.at[0, part], foot_g.at[y, part])
    vol_g[y, zc] = vol_s[y]
    foot_g[y] = foot[0]

    groups = YS * ZS * CS
    member = lax.broadcasted_iota(jnp.int32, (groups, TOTAL), 1)
    owner = lax.broadcasted_iota(jnp.int32, (groups, TOTAL), 0)
    expand = (member // SLOTS == owner).astype(F32).astype(BF16)
    counts = jnp.broadcast_to(count[...].astype(F32), (8, groups)).astype(BF16)
    slot = lax.broadcasted_iota(jnp.int32, (1, TOTAL), 1) % SLOTS
    live = slot.astype(F32) < dot(counts, expand)[0:1]
    block = lax.broadcasted_iota(jnp.int32, (BP, TOTAL), 0)
    offsets = []
    for i in range(YS):
        row = jnp.where(live, off_t[pl.ds(tile_of(i, z, c), 1), :], -1)
        hot[i * BP : (i + 1) * BP, :] = (row == block).astype(F32).astype(BF16)
        offsets.append(row.astype(F32))

    def one_hot_columns():
        rows8 = jnp.concatenate(offsets + [jnp.zeros((8 - YS, TOTAL), F32)], axis=0)
        columns = rows8.T
        block_t = lax.broadcasted_iota(jnp.int32, (TOTAL, CB), 1).astype(F32)
        for i in range(YS):
            hot_t[:, i * CB : (i + 1) * CB] = (columns[:, i : i + 1] == block_t).astype(F32).astype(BF16)
        for h in range(2):
            for i in range(YS):
                back[h, i * CB + BP : (i + 1) * CB, :] = jnp.zeros((CB - BP, SUB), BF16)

    has_lo = (x > 0).astype(F32)
    has_hi = (x < XS - 1).astype(F32)
    lane = lax.broadcasted_iota(jnp.int32, (ROWS_HERE, CB), 1)

    def vertical(b, _):
        cols = pl.ds(pl.multiple_of(b * CB, CB), CB)
        rows_p[b, 0:8, :] = halo_lo[:, cols].astype(F32) * has_lo
        rows_p[b, 8 : 8 + ROWS_HERE, :] = inten[0, :, cols].astype(F32)
        rows_p[b, 8 + ROWS_HERE : 16 + ROWS_HERE, :] = halo_hi[:, cols].astype(F32) * has_hi
        across = taps[RIM] * rows_p[b, 8 : 8 + ROWS_HERE, :]
        for k in range(1, RIM + 1):
            across = across + taps[RIM + k] * (
                rows_p[b, 8 - k : 8 - k + ROWS_HERE, :] + rows_p[b, 8 + k : 8 + k + ROWS_HERE, :]
            )
        rows_a[b + 1] = across
        return 0

    def horizontal(b, _):
        before, here, after = rows_a[b], rows_a[b + 1], rows_a[b + 2]
        smooth = taps[RIM] * here
        for k in range(1, RIM + 1):
            ahead = pltpu.roll(jnp.where(lane < k, after, here), CB - k, 1)
            behind = pltpu.roll(jnp.where(lane >= CB - k, before, here), k, 1)
            smooth = smooth + taps[RIM + k] * (ahead + behind)
        phase = -jnp.log(smooth)
        for q in range(YS):
            for h in range(2):
                first = q * RB + h * HB
                ph_s[q, h, pl.ds(pl.multiple_of(b * HB, HB), HB), :] = phase[first : first + HB]
        return 0

    def smooth_rows(k):
        cols = pl.ds(k * quarter * CB, quarter * CB)
        arrive(halo_lo.at[:, cols], h_send.at[0, k], h_recv.at[0, k], (t, x_from[1]))
        arrive(halo_hi.at[:, cols], h_send.at[1, k], h_recv.at[1, k], (t, x_to[1]))
        lax.fori_loop(k * quarter, (k + 1) * quarter, vertical, 0, unroll=2)

    def phase_part(k):
        lax.fori_loop(k * quarter, (k + 1) * quarter, horizontal, 0, unroll=11)
        span = pl.ds(k * quarter * HB, quarter * HB)
        for d in range(1, YS):
            y_copy(6 + k, d, ph_s.at[y_to[d], 0, span], ph.at[y, 0, span])

    def piece(h, zz, cc):
        return vol_g.at[:, zz * CS + cc, :, halves[h]]

    def give_partner(index, zz, h):
        src = piece(h, zz, c)
        send(src, src, q_send.at[index, h], q_recv.at[index, h], partner)

    def give_partner_sums(index, zz):
        src = cs_g.at[zz * CS + c]
        send(src, src, q_send.at[index, 2], q_recv.at[index, 2], partner)

    def ring_piece(h, p, zz):
        return vol_g.at[pl.ds(2 * p, 2), zz * CS + c, :, halves[h]]

    def ring_send(way, step, h, p, zz):
        src = ring_piece(h, p, zz)
        send(src, src, g_send.at[way, step, h, p], g_recv.at[way, step, h, p], toward[way])

    def z_far(way, step):
        return (z + ZS - step) % ZS if way == 0 else (z + step) % ZS

    def sums_send(way, step, zz):
        src = cs_g.at[zz * CS + c]
        send(src, src, c_send.at[way, step], c_recv.at[way, step], toward[way])

    def serve(step):
        for h in range(2):
            for p in range(2):
                for way in range(2):
                    if step == 4 and way != p:
                        continue
                    zz = z_far(way, step)
                    arrive(
                        ring_piece(h, p, zz), g_send.at[way, step - 1, h, p],
                        g_recv.at[way, step - 1, h, p], toward[1 - way],
                    )
                    if step < 3 or (step == 3 and way == p):
                        ring_send(way, step, h, p, zz)
            for way in range(2 if step < 4 else 1):
                give_partner(step if way == 0 else 4 + step, z_far(way, step), h)
        for way in range(2):
            if step == 4 and way == 1:
                continue
            zz = z_far(way, step)
            arrive(
                cs_g.at[zz * CS + c], c_send.at[way, step - 1], c_recv.at[way, step - 1], toward[1 - way]
            )
            if step < 3 or (step == 3 and way == 0):
                sums_send(way, step, zz)
            give_partner_sums(step if way == 0 else 4 + step, zz)

    rows_a[0] = jnp.zeros((ROWS_HERE, CB), F32)
    rows_a[NCB + 1] = jnp.zeros((ROWS_HERE, CB), F32)
    for h in range(2):
        for d in range(1, YS):
            y_wait(h, d, vol_g.at[y_from[d], zc, :, halves[h]])
        for p in range(2):
            for way in range(2):
                ring_send(way, 0, h, p, z)
        give_partner(0, z, h)
    for d in range(1, YS):
        y_wait(2, d, cs_y.at[y_from[d]])
    cs_g[zc] = cs_y[0] + cs_y[1] + cs_y[2] + cs_y[3]
    for way in range(2):
        sums_send(way, 0, z)
    give_partner_sums(0, z)
    smooth_rows(0)
    smooth_rows(1)
    phase_part(0)
    serve(1)
    smooth_rows(2)
    phase_part(1)
    smooth_rows(3)
    phase_part(2)
    serve(2)
    phase_part(3)
    for d in range(1, YS):
        y_copy(4, d, ph_s.at[y_to[d], 1], ph.at[y, 1])
    ph[y] = ph_s[y]
    for d in range(1, YS):
        y_wait(3, d, foot_g.at[y_from[d], part])
        for e in range(1, XS):
            src = foot_g.at[y_from[d], part]
            send(src, src, x_send.at[d, e], x_recv.at[d, e], (t, x_to[e]))
    serve(3)
    one_hot_columns()
    for d in range(1, YS):
        for e in range(1, XS):
            theirs = pl.ds(pl.multiple_of(x_from[e] * PART, PART), PART)
            arrive(foot_g.at[y_from[d], theirs], x_send.at[d, e], x_recv.at[d, e], (t, x_from[e]))
    serve(4)

    def take_partner(h):
        for index in range(8):
            zz = z_far(0, index) if index < 5 else z_far(1, index - 4)
            arrive(piece(h, zz, 1 - c), q_send.at[index, h], q_recv.at[index, h], partner)
            if h == 1:
                arrive(cs_g.at[zz * CS + 1 - c], q_send.at[index, 2], q_recv.at[index, 2], partner)

    def scales(i, _):
        counted = jnp.sum(hot[pl.ds(pl.multiple_of(i * BP, BP), BP), :].astype(F32), axis=1, keepdims=True)
        sums = dot(ones, foot_g[i])[0:1]
        totals = counted * sums[:, :CB] + pltpu.roll(counted * sums[:, CB:], 1, 0)
        scale_s[i] = 1.0 / jnp.maximum(totals, row_floor)
        return 0

    lax.fori_loop(0, YS, scales, 0)

    def shadows(h):
        take_partner(h)

        def load_row(r, _):
            cols = pl.ds(pl.multiple_of((h * HB + r) * TV, TV), TV)
            got = dot(hot[...], vol_g[:, :, :, cols].reshape(TOTAL, TV)).astype(BF16)
            for i in range(YS):
                loads[i, pl.ds(pl.multiple_of(r * BP, BP), BP), :] = got[i * BP : (i + 1) * BP]
            return 0

        lax.fori_loop(0, HB, load_row, 0)

        def image(i, _):
            images[h, i] = dot(loads[i], foot_g[i])
            return 0

        lax.fori_loop(0, YS, image, 0)

    def weights(h):
        if h == 0:
            for k in range(4):
                span = pl.ds(k * quarter * HB, quarter * HB)
                for d in range(1, YS):
                    y_wait(6 + k, d, ph.at[y_from[d], 0, span])
        else:
            for d in range(1, YS):
                y_wait(4, d, ph.at[y_from[d], 1])

        def one_angle(i, _):
            scale = scale_s[i, :NCB, :]
            for r in range(HB):
                own = images[h, i, r * BP : (r + 1) * BP, :]
                shadow = own[:, :CB] + pltpu.roll(own[:, CB:], 1, 0)
                left_over = ph[i, h, pl.ds(r, NCB, stride=HB), :] - shadow[:NCB]
                res_w[i, h, pl.ds(r, NCB, stride=HB), :] = left_over
                near = jnp.concatenate([left_over * scale, jnp.zeros((BP - NCB, CB), F32)], axis=0)
                far = pltpu.roll(near, BP - 1, 0)
                weigh[r * BP : (r + 1) * BP, :] = jnp.concatenate([near, far], axis=1).astype(BF16)
            spread = dot(weigh[...], foot_g[i], ((1,), (1,)))
            rows = pl.ds(pl.multiple_of(i * CB, CB), BP)
            for r in range(HB):
                given = spread[r * BP : (r + 1) * BP]
                high = given.astype(BF16)
                cols = pl.ds((h * HB + r) * TV, TV)
                back[0, rows, cols] = high
                back[1, rows, cols] = (given - high.astype(F32)).astype(BF16)
            return 0

        lax.fori_loop(0, YS, one_angle, 0)
        for d in range(1, YS):
            y_copy(10 + h, d, res_w.at[y_to[d], h], res_out.at[y, h])
        pltpu.make_async_copy(res_w.at[y, h], res_out.at[y, h], l_sem.at[h]).start()

    def sums_of(h):
        def term_row(r, _):
            cols = pl.ds(pl.multiple_of(r * TV, TV), TV)
            got = dot(hot_t[...], back[0, :, cols]) + dot(hot_t[...], back[1, :, cols])
            terms[:, :, :, :, cols] = got.reshape(YS, ZS, CS, SLOTS, TV)
            return 0

        lax.fori_loop(h * HB, (h + 1) * HB, term_row, 0)
        for off in (4, 3, 5, 2, 6, 1, 7, 0):
            zz = (z + off) % ZS
            send(
                terms.at[:, zz, 1 - c, :, halves[h]], pair_r.at[h, zz],
                p_send.at[off, h], p_recv.at[off, h], partner,
            )

    def add_pair(off, h):
        zz = (z + off) % ZS
        arrive(pair_r.at[h, zz], p_send.at[off, h], p_recv.at[off, h], partner)
        terms[:, zz, c, :, halves[h]] = terms[:, zz, c, :, halves[h]] + pair_r[h, zz]

    def add_ring(way, step, h, d, zz):
        got = ring_r.at[h, way, step, d]
        arrive(got, r_send.at[h, way, step, d], r_recv.at[h, way, step, d], toward[1 - way])
        mine = y_to[d]
        terms[mine, zz, c, :, halves[h]] = terms[mine, zz, c, :, halves[h]] + ring_r[h, way, step, d]

    def sum_step(h, step):
        for way in range(2):
            if step > 0 or way == 0:
                add_pair(4 - step if way == 0 else 4 + step, h)
        for e in range(2):
            for way in range(2):
                for p in range(2):
                    if step == 0 and p != way:
                        continue
                    d = 2 * p + e
                    zz = (z + 4 - step) % ZS if way == 0 else (z + 4 + step) % ZS
                    if step > 1 or (step == 1 and p == way):
                        add_ring(way, step - 1, h, d, zz)
                    send(
                        terms.at[y_to[d], zz, c, :, halves[h]], ring_r.at[h, way, step, d],
                        r_send.at[h, way, step, d], r_recv.at[h, way, step, d], toward[way],
                    )
        if step == 2:
            add_pair(0, h)

    def sum_end(h):
        for d in (2, 1, 3, 0):
            for way in range(2):
                add_ring(way, 3, h, d, z)
            if d > 0:
                y_copy(12 + h, d, terms.at[y_to[d], z, c, :, halves[h]], fin.at[h, y])
        fin[h, y] = terms[y, z, c, :, halves[h]]

    shadows(0)
    weights(0)
    sums_of(0)
    sum_step(0, 0)
    shadows(1)
    sum_step(0, 1)
    weights(1)
    sums_of(1)
    sum_step(0, 2)
    sum_step(1, 0)
    sum_step(0, 3)
    sum_step(1, 1)
    sum_step(1, 2)
    sum_end(0)
    sum_step(1, 3)
    total = cs_g[0]
    for k in range(1, ZS * CS):
        total = total + cs_g[k]
    col_out[...] = 1.0 / total
    sum_end(1)
    for h in range(2):
        for d in range(1, YS):
            y_wait(10 + h, d, res_out.at[y_from[d], h])
        for d in range(1, YS):
            y_wait(12 + h, d, fin.at[h, y_from[d]])
        cor_out[h] = fin[h]
        pltpu.make_async_copy(res_w.at[y, h], res_out.at[y, h], l_sem.at[h]).wait()
    for copy in started:
        copy.wait_send()


def finish(res, cor, col, res_out, cor_out):
    for h in range(2):
        for b in range(NCB):
            res_out[0, h * HB : (h + 1) * HB, b * CB : (b + 1) * CB] = res[0, h, b * HB : (b + 1) * HB, :]
        for r in range(HB):
            cor_out[:, h * HB + r, :] = cor[h, 0, :, r * TV : (r + 1) * TV] * col[...]


def local(intensity, volume, footprint, foot_offset, tile_count):
    dma = pltpu.SemaphoreType.DMA
    vmem = pl.BlockSpec(memory_space=pltpu.VMEM)
    hbm = pl.BlockSpec(memory_space=pl.ANY)
    residual, summed, columns = pl.pallas_call(
        kernel,
        out_shape=(
            jax.ShapeDtypeStruct((YS, 2, HR, CB), F32),
            jax.ShapeDtypeStruct((2, YS, SLOTS, HS), F32),
            jax.ShapeDtypeStruct((8, TV), F32),
        ),
        in_specs=[hbm] + [vmem] * 4,
        out_specs=(hbm, vmem, vmem),
        scratch_shapes=[
            pltpu.VMEM((1, ROWS_HERE, NCB * CB), BF16),
            pltpu.VMEM((YS, SLOTS, SUB), BF16),
            pltpu.VMEM((YS, ZS * CS, SLOTS, SUB), BF16),
            pltpu.VMEM((YS, TV, TV), BF16),
            pltpu.VMEM((YS, 8, TV), F32),
            pltpu.VMEM((ZS * CS, 8, TV), F32),
            pltpu.VMEM((8, NCB * CB), BF16),
            pltpu.VMEM((8, NCB * CB), BF16),
            pltpu.VMEM((NCB, ROWS_HERE + 16, CB), F32),
            pltpu.VMEM((NCB + 2, ROWS_HERE, CB), F32),
            pltpu.VMEM((YS, 2, HR, CB), F32),
            pltpu.VMEM((YS, 2, HR, CB), F32),
            pltpu.VMEM((YS * BP, TOTAL), BF16),
            pltpu.VMEM((TOTAL, YS * CB), BF16),
            pltpu.VMEM((YS, HB * BP, TV), BF16),
            pltpu.VMEM((2, YS, HB * BP, TV), F32),
            pltpu.VMEM((YS, BP, CB), F32),
            pltpu.VMEM((HB * BP, TV), BF16),
            pltpu.VMEM((YS, 2, HR, CB), F32),
            pltpu.VMEM((2, YS * CB, SUB), BF16),
            pltpu.VMEM((YS, ZS, CS, SLOTS, SUB), F32),
            pltpu.VMEM((2, ZS, YS, SLOTS, HS), F32),
            pltpu.VMEM((2, 2, 4, YS, SLOTS, HS), F32),
            pltpu.VMEM((2, YS, SLOTS, HS), F32),
            dma((14, 4)), dma((14, 4)),
            dma((2, 4)), dma((2, 4)),
            dma((4, 4)), dma((4, 4)),
            dma((2, 4, 2, 2)), dma((2, 4, 2, 2)),
            dma((2, 4)), dma((2, 4)),
            dma((8, 3)), dma((8, 3)),
            dma((8, 2)), dma((8, 2)),
            dma((2, 2, 4, 4)), dma((2, 2, 4, 4)),
            dma((3,)),
        ],
        compiler_params=pltpu.CompilerParams(
            collective_id=0, has_side_effects=True, vmem_limit_bytes=60 << 20
        ),
        name="sirt",
    )(intensity, volume, footprint, foot_offset.T, tile_count.reshape(1, -1))
    return pl.pallas_call(
        finish,
        grid=(YS,),
        out_shape=(
            jax.ShapeDtypeStruct((1, ROWS_HERE, NCB * CB), F32),
            jax.ShapeDtypeStruct((SLOTS, ROWS_HERE, TV), F32),
        ),
        in_specs=[
            pl.BlockSpec((1, 2, HR, CB), lambda q: (q, 0, 0, 0)),
            pl.BlockSpec((2, 1, SLOTS, HS), lambda q: (0, q, 0, 0)),
            pl.BlockSpec((8, TV), lambda q: (0, 0)),
        ],
        out_specs=(
            pl.BlockSpec((1, RB, NCB * CB), lambda q: (0, q, 0)),
            pl.BlockSpec((SLOTS, RB, TV), lambda q: (0, q, 0)),
        ),
        name="finish",
    )(residual, summed, columns)


def solution(mesh):
    placed = (P("tile", "row", None), P("tile", "row", None), P("tile", None, None), P(), P())
    return jax.shard_map(
        local,
        mesh=mesh,
        in_specs=placed,
        out_specs=(P("tile", "row", None), P("tile", "row", None)),
        check_vma=False,
    )
```

```python
import functools

import jax
import jax.numpy as jnp
import numpy as np
from jax import lax
from jax.experimental import pallas as pl
from jax.experimental.pallas import tpu as pltpu
from jax.sharding import PartitionSpec as P

RIM = 3
NCB = 88
CB = 128
TV = 256
YS, ZS, CS, XS = 4, 8, 2, 4
SLOTS = 8
RB = 8
SUB = RB * TV
TOTAL = YS * ZS * CS * SLOTS
BP = 96
PART = TV // XS
HB = RB // 2
HR = NCB * HB
HS = HB * TV
ROWS_HERE = YS * RB

decay_length = 2.0
row_floor = 0.5

F32 = jnp.float32
BF16 = jnp.bfloat16
MESH = pl.DeviceIdType.MESH


def smoothing_taps():
    spread_taps = np.exp(-np.abs(np.arange(-RIM, RIM + 1)) / decay_length)
    return [float(t) for t in (spread_taps / spread_taps.sum()).astype(np.float32)]


def dot(a, b, dims=((1,), (0,))):
    return lax.dot_general(a, b, (dims, ((), ())), preferred_element_type=F32)


def kernel(
    inten_h, vol, foot, off_t, count,
    res_out, cor_out, col_out,
    inten, vol_s, vol_g, foot_g, cs_y, cs_g,
    halo_lo, halo_hi, rows_p, rows_a, ph_s, ph,
    hot, hot_t, loads, images, scale_s, weigh, res_w, back, terms, pair_r, ring_r, fin,
    y_send, y_recv, h_send, h_recv, x_send, x_recv, g_send, g_recv, c_send, c_recv,
    q_send, q_recv, p_send, p_recv, r_send, r_recv, l_sem,
):
    taps = smoothing_taps()
    t = lax.axis_index("tile")
    x = lax.axis_index("row")
    y = t // (ZS * CS)
    zc = t % (ZS * CS)
    z = zc // CS
    c = zc % CS

    def tile_of(yy, zz, cc):
        return (yy * ZS + zz) * CS + cc

    def device(yy, zz, cc):
        return (tile_of(yy, zz, cc), x)

    z_up, z_down = (z + 1) % ZS, (z + ZS - 1) % ZS
    partner = device(y, z, 1 - c)
    toward = (device(y, z_up, c), device(y, z_down, c))
    y_to = [(y + d) % YS for d in range(YS)]
    y_from = [(y + YS - d) % YS for d in range(YS)]
    x_to = [(x + d) % XS for d in range(XS)]
    x_from = [(x + XS - d) % XS for d in range(XS)]

    load_inten = pltpu.make_async_copy(inten_h, inten, l_sem.at[2])
    load_inten.start()

    barrier = pltpu.get_barrier_semaphore()
    peers = [device(y_to[d], z, c) for d in range(1, YS)]
    peers += [device(y, zz, c) for zz in (z_up, z_down)]
    peers += [(t, x_to[d]) for d in range(1, XS)] + [partner]
    for peer in peers:
        pl.semaphore_signal(barrier, inc=1, device_id=peer, device_id_type=MESH)

    for q in range(YS):
        for r in range(RB):
            vol_s[q, :, r * TV : (r + 1) * TV] = vol[:, q * RB + r, :].astype(BF16)
    pl.semaphore_wait(barrier, len(peers))

    started = []

    def send(src, dst, ssem, rsem, dev):
        copy = pltpu.make_async_remote_copy(
            src_ref=src, dst_ref=dst, send_sem=ssem, recv_sem=rsem,
            device_id=dev, device_id_type=MESH,
        )
        copy.start()
        started.append(copy)

    def arrive(dst, ssem, rsem, dev):
        pltpu.make_async_remote_copy(
            src_ref=dst, dst_ref=dst, send_sem=ssem, recv_sem=rsem,
            device_id=dev, device_id_type=MESH,
        ).wait_recv()

    def y_copy(kind, d, src, dst):
        send(src, dst, y_send.at[kind, d], y_recv.at[kind, d], device(y_to[d], z, c))

    def y_wait(kind, d, dst):
        arrive(dst, y_send.at[kind, d], y_recv.at[kind, d], device(y_from[d], z, c))

    halves = [pl.ds(0, HS), pl.ds(HS, HS)]

    for h in range(2):
        for d in range(1, YS):
            y_copy(h, d, vol_s.at[y_to[d], :, halves[h]], vol_g.at[y, zc, :, halves[h]])
    quarter = NCB // 4
    load_inten.wait()
    for k in range(4):
        cols = pl.ds(k * quarter * CB, quarter * CB)
        send(
            inten.at[0, pl.ds(ROWS_HERE - 8, 8), cols], halo_lo.at[:, cols],
            h_send.at[0, k], h_recv.at[0, k], (t, x_to[1]),
        )
        send(inten.at[0, pl.ds(0, 8), cols], halo_hi.at[:, cols], h_send.at[1, k], h_recv.at[1, k], (t, x_from[1]))
    ones = jnp.ones((8, TV), BF16)
    cs_y[y] = dot(ones, foot[0], ((1,), (1,)))
    for d in range(1, YS):
        y_copy(2, d, cs_y.at[y], cs_y.at[y])
    part = pl.ds(pl.multiple_of(x * PART, PART), PART)
    for d in range(1, YS):
        y_copy(3, d, foot.at[0, part], foot_g.at[y, part])
    vol_g[y, zc] = vol_s[y]
    foot_g[y] = foot[0]

    groups = YS * ZS * CS
    member = lax.broadcasted_iota(jnp.int32, (groups, TOTAL), 1)
    owner = lax.broadcasted_iota(jnp.int32, (groups, TOTAL), 0)
    expand = (member // SLOTS == owner).astype(F32).astype(BF16)
    counts = jnp.broadcast_to(count[...].astype(F32), (8, groups)).astype(BF16)
    slot = lax.broadcasted_iota(jnp.int32, (1, TOTAL), 1) % SLOTS
    live = slot.astype(F32) < dot(counts, expand)[0:1]
    block = lax.broadcasted_iota(jnp.int32, (BP, TOTAL), 0)
    offsets = []
    for i in range(YS):
        row = jnp.where(live, off_t[pl.ds(tile_of(i, z, c), 1), :], -1)
        hot[i * BP : (i + 1) * BP, :] = (row == block).astype(F32).astype(BF16)
        offsets.append(row.astype(F32))

    def one_hot_columns():
        rows8 = jnp.concatenate(offsets + [jnp.zeros((8 - YS, TOTAL), F32)], axis=0)
        columns = rows8.T
        block_t = lax.broadcasted_iota(jnp.int32, (TOTAL, CB), 1).astype(F32)
        for i in range(YS):
            hot_t[:, i * CB : (i + 1) * CB] = (columns[:, i : i + 1] == block_t).astype(F32).astype(BF16)
        for h in range(2):
            for i in range(YS):
                back[h, i * CB + BP : (i + 1) * CB, :] = jnp.zeros((CB - BP, SUB), BF16)

    has_lo = (x > 0).astype(F32)
    has_hi = (x < XS - 1).astype(F32)
    lane = lax.broadcasted_iota(jnp.int32, (ROWS_HERE, CB), 1)

    def vertical(b, _):
        cols = pl.ds(pl.multiple_of(b * CB, CB), CB)
        rows_p[b, 0:8, :] = halo_lo[:, cols].astype(F32) * has_lo
        rows_p[b, 8 : 8 + ROWS_HERE, :] = inten[0, :, cols].astype(F32)
        rows_p[b, 8 + ROWS_HERE : 16 + ROWS_HERE, :] = halo_hi[:, cols].astype(F32) * has_hi
        across = taps[RIM] * rows_p[b, 8 : 8 + ROWS_HERE, :]
        for k in range(1, RIM + 1):
            across = across + taps[RIM + k] * (
                rows_p[b, 8 - k : 8 - k + ROWS_HERE, :] + rows_p[b, 8 + k : 8 + k + ROWS_HERE, :]
            )
        rows_a[b + 1] = across
        return 0

    def horizontal(b, _):
        before, here, after = rows_a[b], rows_a[b + 1], rows_a[b + 2]
        smooth = taps[RIM] * here
        for k in range(1, RIM + 1):
            ahead = pltpu.roll(jnp.where(lane < k, after, here), CB - k, 1)
            behind = pltpu.roll(jnp.where(lane >= CB - k, before, here), k, 1)
            smooth = smooth + taps[RIM + k] * (ahead + behind)
        phase = -jnp.log(smooth)
        for q in range(YS):
            for h in range(2):
                first = q * RB + h * HB
                ph_s[q, h, pl.ds(pl.multiple_of(b * HB, HB), HB), :] = phase[first : first + HB]
        return 0

    def smooth_rows(k):
        cols = pl.ds(k * quarter * CB, quarter * CB)
        arrive(halo_lo.at[:, cols], h_send.at[0, k], h_recv.at[0, k], (t, x_from[1]))
        arrive(halo_hi.at[:, cols], h_send.at[1, k], h_recv.at[1, k], (t, x_to[1]))
        lax.fori_loop(k * quarter, (k + 1) * quarter, vertical, 0, unroll=2)

    def phase_part(k):
        lax.fori_loop(k * quarter, (k + 1) * quarter, horizontal, 0, unroll=11)
        span = pl.ds(k * quarter * HB, quarter * HB)
        for d in range(1, YS):
            y_copy(6 + k, d, ph_s.at[y_to[d], 0, span], ph.at[y, 0, span])

    def piece(h, zz, cc):
        return vol_g.at[:, zz * CS + cc, :, halves[h]]

    def give_partner(index, zz, h):
        src = piece(h, zz, c)
        send(src, src, q_send.at[index, h], q_recv.at[index, h], partner)

    def give_partner_sums(index, zz):
        src = cs_g.at[zz * CS + c]
        send(src, src, q_send.at[index, 2], q_recv.at[index, 2], partner)

    def ring_piece(h, p, zz):
        return vol_g.at[pl.ds(2 * p, 2), zz * CS + c, :, halves[h]]

    def ring_send(way, step, h, p, zz):
        src = ring_piece(h, p, zz)
        send(src, src, g_send.at[way, step, h, p], g_recv.at[way, step, h, p], toward[way])

    def z_far(way, step):
        return (z + ZS - step) % ZS if way == 0 else (z + step) % ZS

    def sums_send(way, step, zz):
        src = cs_g.at[zz * CS + c]
        send(src, src, c_send.at[way, step], c_recv.at[way, step], toward[way])

    def serve(step):
        for h in range(2):
            for p in range(2):
                for way in range(2):
                    if step == 4 and way != p:
                        continue
                    zz = z_far(way, step)
                    arrive(
                        ring_piece(h, p, zz), g_send.at[way, step - 1, h, p],
                        g_recv.at[way, step - 1, h, p], toward[1 - way],
                    )
                    if step < 3 or (step == 3 and way == p):
                        ring_send(way, step, h, p, zz)
            for way in range(2 if step < 4 else 1):
                give_partner(step if way == 0 else 4 + step, z_far(way, step), h)
        for way in range(2):
            if step == 4 and way == 1:
                continue
            zz = z_far(way, step)
            arrive(
                cs_g.at[zz * CS + c], c_send.at[way, step - 1], c_recv.at[way, step - 1], toward[1 - way]
            )
            if step < 3 or (step == 3 and way == 0):
                sums_send(way, step, zz)
            give_partner_sums(step if way == 0 else 4 + step, zz)

    rows_a[0] = jnp.zeros((ROWS_HERE, CB), F32)
    rows_a[NCB + 1] = jnp.zeros((ROWS_HERE, CB), F32)
    for h in range(2):
        for d in range(1, YS):
            y_wait(h, d, vol_g.at[y_from[d], zc, :, halves[h]])
        for p in range(2):
            for way in range(2):
                ring_send(way, 0, h, p, z)
        give_partner(0, z, h)
    for d in range(1, YS):
        y_wait(2, d, cs_y.at[y_from[d]])
    cs_g[zc] = cs_y[0] + cs_y[1] + cs_y[2] + cs_y[3]
    for way in range(2):
        sums_send(way, 0, z)
    give_partner_sums(0, z)
    smooth_rows(0)
    smooth_rows(1)
    phase_part(0)
    serve(1)
    smooth_rows(2)
    phase_part(1)
    smooth_rows(3)
    phase_part(2)
    serve(2)
    phase_part(3)
    for d in range(1, YS):
        y_copy(4, d, ph_s.at[y_to[d], 1], ph.at[y, 1])
    ph[y] = ph_s[y]
    for d in range(1, YS):
        y_wait(3, d, foot_g.at[y_from[d], part])
        for e in range(1, XS):
            src = foot_g.at[y_from[d], part]
            send(src, src, x_send.at[d, e], x_recv.at[d, e], (t, x_to[e]))
    serve(3)
    one_hot_columns()
    for d in range(1, YS):
        for e in range(1, XS):
            theirs = pl.ds(pl.multiple_of(x_from[e] * PART, PART), PART)
            arrive(foot_g.at[y_from[d], theirs], x_send.at[d, e], x_recv.at[d, e], (t, x_from[e]))
    serve(4)

    def take_partner(h):
        for index in range(8):
            zz = z_far(0, index) if index < 5 else z_far(1, index - 4)
            arrive(piece(h, zz, 1 - c), q_send.at[index, h], q_recv.at[index, h], partner)
            if h == 1:
                arrive(cs_g.at[zz * CS + 1 - c], q_send.at[index, 2], q_recv.at[index, 2], partner)

    def scales(i, _):
        counted = jnp.sum(hot[pl.ds(pl.multiple_of(i * BP, BP), BP), :].astype(F32), axis=1, keepdims=True)
        sums = dot(ones, foot_g[i])[0:1]
        totals = counted * sums[:, :CB] + pltpu.roll(counted * sums[:, CB:], 1, 0)
        scale_s[i] = 1.0 / jnp.maximum(totals, row_floor)
        return 0

    lax.fori_loop(0, YS, scales, 0)

    def shadows(h):
        take_partner(h)

        def load_row(r, _):
            cols = pl.ds(pl.multiple_of((h * HB + r) * TV, TV), TV)
            got = dot(hot[...], vol_g[:, :, :, cols].reshape(TOTAL, TV)).astype(BF16)
            for i in range(YS):
                loads[i, pl.ds(pl.multiple_of(r * BP, BP), BP), :] = got[i * BP : (i + 1) * BP]
            return 0

        lax.fori_loop(0, HB, load_row, 0)

        def image(i, _):
            images[h, i] = dot(loads[i], foot_g[i])
            return 0

        lax.fori_loop(0, YS, image, 0)

    def weights(h):
        if h == 0:
            for k in range(4):
                span = pl.ds(k * quarter * HB, quarter * HB)
                for d in range(1, YS):
                    y_wait(6 + k, d, ph.at[y_from[d], 0, span])
        else:
            for d in range(1, YS):
                y_wait(4, d, ph.at[y_from[d], 1])

        def one_angle(i, _):
            scale = scale_s[i, :NCB, :]
            for r in range(HB):
                own = images[h, i, r * BP : (r + 1) * BP, :]
                shadow = own[:, :CB] + pltpu.roll(own[:, CB:], 1, 0)
                left_over = ph[i, h, pl.ds(r, NCB, stride=HB), :] - shadow[:NCB]
                res_w[i, h, pl.ds(r, NCB, stride=HB), :] = left_over
                near = jnp.concatenate([left_over * scale, jnp.zeros((BP - NCB, CB), F32)], axis=0)
                far = pltpu.roll(near, BP - 1, 0)
                weigh[r * BP : (r + 1) * BP, :] = jnp.concatenate([near, far], axis=1).astype(BF16)
            spread = dot(weigh[...], foot_g[i], ((1,), (1,)))
            rows = pl.ds(pl.multiple_of(i * CB, CB), BP)
            for r in range(HB):
                given = spread[r * BP : (r + 1) * BP]
                high = given.astype(BF16)
                cols = pl.ds((h * HB + r) * TV, TV)
                back[0, rows, cols] = high
                back[1, rows, cols] = (given - high.astype(F32)).astype(BF16)
            return 0

        lax.fori_loop(0, YS, one_angle, 0)
        for d in range(1, YS):
            y_copy(10 + h, d, res_w.at[y_to[d], h], res_out.at[y, h])
        pltpu.make_async_copy(res_w.at[y, h], res_out.at[y, h], l_sem.at[h]).start()

    def sums_of(h):
        def term_row(r, _):
            cols = pl.ds(pl.multiple_of(r * TV, TV), TV)
            got = dot(hot_t[...], back[0, :, cols]) + dot(hot_t[...], back[1, :, cols])
            terms[:, :, :, :, cols] = got.reshape(YS, ZS, CS, SLOTS, TV)
            return 0

        lax.fori_loop(h * HB, (h + 1) * HB, term_row, 0)
        for off in (4, 3, 5, 2, 6, 1, 7, 0):
            zz = (z + off) % ZS
            send(
                terms.at[:, zz, 1 - c, :, halves[h]], pair_r.at[h, zz],
                p_send.at[off, h], p_recv.at[off, h], partner,
            )

    def add_pair(off, h):
        zz = (z + off) % ZS
        arrive(pair_r.at[h, zz], p_send.at[off, h], p_recv.at[off, h], partner)
        terms[:, zz, c, :, halves[h]] = terms[:, zz, c, :, halves[h]] + pair_r[h, zz]

    def add_ring(way, step, h, d, zz):
        got = ring_r.at[h, way, step, d]
        arrive(got, r_send.at[h, way, step, d], r_recv.at[h, way, step, d], toward[1 - way])
        mine = y_to[d]
        terms[mine, zz, c, :, halves[h]] = terms[mine, zz, c, :, halves[h]] + ring_r[h, way, step, d]

    def sum_step(h, step):
        for way in range(2):
            if step > 0 or way == 0:
                add_pair(4 - step if way == 0 else 4 + step, h)
        for e in range(2):
            for way in range(2):
                for p in range(2):
                    if step == 0 and p != way:
                        continue
                    d = 2 * p + e
                    zz = (z + 4 - step) % ZS if way == 0 else (z + 4 + step) % ZS
                    if step > 1 or (step == 1 and p == way):
                        add_ring(way, step - 1, h, d, zz)
                    send(
                        terms.at[y_to[d], zz, c, :, halves[h]], ring_r.at[h, way, step, d],
                        r_send.at[h, way, step, d], r_recv.at[h, way, step, d], toward[way],
                    )
        if step == 2:
            add_pair(0, h)

    def sum_end(h):
        for d in (2, 1, 3, 0):
            for way in range(2):
                add_ring(way, 3, h, d, z)
            if d > 0:
                y_copy(12 + h, d, terms.at[y_to[d], z, c, :, halves[h]], fin.at[h, y])
        fin[h, y] = terms[y, z, c, :, halves[h]]

    shadows(0)
    weights(0)
    sums_of(0)
    sum_step(0, 0)
    shadows(1)
    weights(1)
    sums_of(1)
    sum_step(0, 1)
    sum_step(1, 0)
    sum_step(0, 2)
    sum_step(1, 1)
    sum_step(0, 3)
    sum_step(1, 2)
    sum_end(0)
    sum_step(1, 3)
    total = cs_g[0]
    for k in range(1, ZS * CS):
        total = total + cs_g[k]
    col_out[...] = 1.0 / total
    sum_end(1)
    for h in range(2):
        for d in range(1, YS):
            y_wait(10 + h, d, res_out.at[y_from[d], h])
        for d in range(1, YS):
            y_wait(12 + h, d, fin.at[h, y_from[d]])
        cor_out[h] = fin[h]
        pltpu.make_async_copy(res_w.at[y, h], res_out.at[y, h], l_sem.at[h]).wait()
    for copy in started:
        copy.wait_send()


def finish(res, cor, col, res_out, cor_out):
    for h in range(2):
        for b in range(NCB):
            res_out[0, h * HB : (h + 1) * HB, b * CB : (b + 1) * CB] = res[0, h, b * HB : (b + 1) * HB, :]
        for r in range(HB):
            cor_out[:, h * HB + r, :] = cor[h, 0, :, r * TV : (r + 1) * TV] * col[...]


def local(intensity, volume, footprint, foot_offset, tile_count):
    dma = pltpu.SemaphoreType.DMA
    vmem = pl.BlockSpec(memory_space=pltpu.VMEM)
    hbm = pl.BlockSpec(memory_space=pl.ANY)
    residual, summed, columns = pl.pallas_call(
        kernel,
        out_shape=(
            jax.ShapeDtypeStruct((YS, 2, HR, CB), F32),
            jax.ShapeDtypeStruct((2, YS, SLOTS, HS), F32),
            jax.ShapeDtypeStruct((8, TV), F32),
        ),
        in_specs=[hbm] + [vmem] * 4,
        out_specs=(hbm, vmem, vmem),
        scratch_shapes=[
            pltpu.VMEM((1, ROWS_HERE, NCB * CB), BF16),
            pltpu.VMEM((YS, SLOTS, SUB), BF16),
            pltpu.VMEM((YS, ZS * CS, SLOTS, SUB), BF16),
            pltpu.VMEM((YS, TV, TV), BF16),
            pltpu.VMEM((YS, 8, TV), F32),
            pltpu.VMEM((ZS * CS, 8, TV), F32),
            pltpu.VMEM((8, NCB * CB), BF16),
            pltpu.VMEM((8, NCB * CB), BF16),
            pltpu.VMEM((NCB, ROWS_HERE + 16, CB), F32),
            pltpu.VMEM((NCB + 2, ROWS_HERE, CB), F32),
            pltpu.VMEM((YS, 2, HR, CB), F32),
            pltpu.VMEM((YS, 2, HR, CB), F32),
            pltpu.VMEM((YS * BP, TOTAL), BF16),
            pltpu.VMEM((TOTAL, YS * CB), BF16),
            pltpu.VMEM((YS, HB * BP, TV), BF16),
            pltpu.VMEM((2, YS, HB * BP, TV), F32),
            pltpu.VMEM((YS, BP, CB), F32),
            pltpu.VMEM((HB * BP, TV), BF16),
            pltpu.VMEM((YS, 2, HR, CB), F32),
            pltpu.VMEM((2, YS * CB, SUB), BF16),
            pltpu.VMEM((YS, ZS, CS, SLOTS, SUB), F32),
            pltpu.VMEM((2, ZS, YS, SLOTS, HS), F32),
            pltpu.VMEM((2, 2, 4, YS, SLOTS, HS), F32),
            pltpu.VMEM((2, YS, SLOTS, HS), F32),
            dma((14, 4)), dma((14, 4)),
            dma((2, 4)), dma((2, 4)),
            dma((4, 4)), dma((4, 4)),
            dma((2, 4, 2, 2)), dma((2, 4, 2, 2)),
            dma((2, 4)), dma((2, 4)),
            dma((8, 3)), dma((8, 3)),
            dma((8, 2)), dma((8, 2)),
            dma((2, 2, 4, 4)), dma((2, 2, 4, 4)),
            dma((3,)),
        ],
        compiler_params=pltpu.CompilerParams(
            collective_id=0, has_side_effects=True, vmem_limit_bytes=60 << 20
        ),
        name="sirt",
    )(intensity, volume, footprint, foot_offset.T, tile_count.reshape(1, -1))
    return pl.pallas_call(
        finish,
        grid=(YS,),
        out_shape=(
            jax.ShapeDtypeStruct((1, ROWS_HERE, NCB * CB), F32),
            jax.ShapeDtypeStruct((SLOTS, ROWS_HERE, TV), F32),
        ),
        in_specs=[
            pl.BlockSpec((1, 2, HR, CB), lambda q: (q, 0, 0, 0)),
            pl.BlockSpec((2, 1, SLOTS, HS), lambda q: (0, q, 0, 0)),
            pl.BlockSpec((8, TV), lambda q: (0, 0)),
        ],
        out_specs=(
            pl.BlockSpec((1, RB, NCB * CB), lambda q: (0, q, 0)),
            pl.BlockSpec((SLOTS, RB, TV), lambda q: (0, q, 0)),
        ),
        name="finish",
    )(residual, summed, columns)


def solution(mesh):
    placed = (P("tile", "row", None), P("tile", "row", None), P("tile", None, None), P(), P())
    return jax.shard_map(
        local,
        mesh=mesh,
        in_specs=placed,
        out_specs=(P("tile", "row", None), P("tile", "row", None)),
        check_vma=False,
    )
```
